32 devices in a mesh: af: 4 (over z), gx: 2 (over x), gy: 4 (over y, core).
Axes of the slice: x: 2, y: 2, z: 4, core: 2. Of those that a mesh axis runs over, the one named last changes fastest.
Arguments:
- source: float32 [4, 2048, 2048], P('af', ('gx', 'gy')), parts along dimension 0, may hold values from -0.8 to 0.8
- screening: float32 [4], P('af'), parts along dimension 0, may hold values from 0.0002 to 0.002
Outputs:
- solution: float32 [4, 2048, 2048], P('af', ('gx', 'gy')), parts along dimension 0
The draws below stay inside these ranges and needn't reach their ends.
There are 4 independent parts, one for each index of `af`. The reference program is written for one: setup_inputs(seed, part) draws one part's arguments, and reference() takes and returns one part's arrays. A program takes and returns all parts, laid end to end along the dimension named above; each array names one. Nothing has to cross between parts.
All inputs are finite; a program needn't handle non-finite values.
Results may differ from the reference program's by a relative error of at most 0.0014.
Values sent between devices are 32-bit elements; how exact they have to be, the bound alone decides.
A program may use at most 128 MiB of HBM per device.

```python
import math
import jax
import jax.numpy as jnp
from jax import lax

FIELDS = 1
NX = 2048
NY = 2048
N_GX = 2
N_GY = 4


def draw_source(key, part):
    rough_key = jax.random.fold_in(key, 0)
    return jnp.clip(0.1 * jax.random.normal(rough_key, (FIELDS, NX, NY), jnp.float32), -0.6, 0.6)


def setup_inputs(seed: int = 0, part: int = 0) -> dict:
    arg_keys = jax.random.split(jax.random.key(seed), 3)
    part_keys = jax.random.split(jax.random.fold_in(arg_keys[2], part), 3)
    return {
        "source": draw_source(jax.random.fold_in(jax.random.fold_in(arg_keys[2], part), 71), part),
        "screening": jnp.clip(jnp.exp(jax.random.uniform(part_keys[1], (FIELDS,), jnp.float32, math.log(0.0002), math.log(0.002))), 0.0002, 0.002),
    }


HIGHEST = lax.Precision.HIGHEST

def sine_table(length):
    numbers = jnp.arange(length, dtype=jnp.int32) + 1
    phases = numbers[:, None] * numbers[None, :] % (2 * length + 2)
    return math.sqrt(2.0 / (length + 1)) * jnp.sin(phases.astype(jnp.float32) * (math.pi / (length + 1)))

def diagonal_factor(screening, length):
    numbers = (jnp.arange(length, dtype=jnp.int32) + 1).astype(jnp.float32)
    return 4.0 + screening[:, None] - 2.0 * jnp.cos(numbers * (math.pi / (length + 1)))[None, :]

def shift_rows(values, offset, fill_value):
    row_count = values.shape[-2]
    pad_shape = values.shape[:-2] + (abs(offset), values.shape[-1])
    padding = jnp.full(pad_shape, fill_value, values.dtype)
    if offset > 0:
        return jnp.concatenate([padding, values[..., :row_count - offset, :]], axis=-2)
    return jnp.concatenate([values[..., -offset:, :], padding], axis=-2)

def cyclic_solve(low_band, middle, up_band, all_sides):
    row_count = middle.shape[-2]
    stride = 1
    while stride < row_count:
        left_ratio = low_band / shift_rows(middle, stride, 1.0)
        right_ratio = up_band / shift_rows(middle, -stride, 1.0)
        next_low = -left_ratio * shift_rows(low_band, stride, 0.0)
        next_up = -right_ratio * shift_rows(up_band, -stride, 0.0)
        middle = middle - left_ratio * shift_rows(up_band, stride, 0.0) - right_ratio * shift_rows(low_band, -stride, 0.0)
        all_sides = tuple((each_side - left_ratio * shift_rows(each_side, stride, 0.0) - right_ratio * shift_rows(each_side, -stride, 0.0) for each_side in all_sides))
        low_band, up_band = (next_low, next_up)
        stride *= 2
    return tuple((each_side / middle for each_side in all_sides))

def reference(source, screening):
    fields = source.shape[0]
    groups = N_GX * N_GY
    kept_lines = NY // (2 * groups)
    inner_lines = kept_lines - 1
    transform = sine_table(NX)
    spectrum = jnp.einsum('fiy,ki->fyk', source, transform, precision=HIGHEST)
    paired = spectrum.reshape(fields, NY // 2, 2, NX)
    even_lines = paired[:, :, 0, :]
    odd_lines = paired[:, :, 1, :]
    factor = diagonal_factor(screening, NX)[:, None, :]
    later_even = jnp.concatenate([even_lines[:, 1:, :], jnp.zeros_like(even_lines[:, :1, :])], axis=1)
    reduced = (even_lines + factor * odd_lines + later_even).reshape(fields, groups, kept_lines, NX)
    center = (factor * factor - 2.0)[:, None, :, :]
    band_shape = (fields, groups, inner_lines, NX)
    row_index = lax.broadcasted_iota(jnp.int32, band_shape, 2)
    low_band = jnp.where(row_index > 0, -1.0, 0.0)
    up_band = jnp.where(row_index < inner_lines - 1, -1.0, 0.0)
    middle = jnp.broadcast_to(center, band_shape)
    first_unit = jnp.where(row_index == 0, 1.0, 0.0)
    last_unit = jnp.where(row_index == inner_lines - 1, 1.0, 0.0)
    base_part, left_spike, right_spike = cyclic_solve(low_band, middle, up_band, (reduced[:, :, :inner_lines, :], first_unit, last_unit))
    sides_all = reduced[:, :, inner_lines, :] + base_part[:, :, inner_lines - 1, :]
    heads_all = base_part[:, :, 0, :]
    later_heads = jnp.concatenate([heads_all[:, 1:, :], jnp.zeros_like(heads_all[:, :1, :])], axis=1)
    chain_side = sides_all + later_heads
    tail_left = left_spike[:, 0, inner_lines - 1, :][:, None, :]
    head_left = left_spike[:, 0, 0, :][:, None, :]
    head_right = right_spike[:, 0, 0, :][:, None, :]
    tail_right = right_spike[:, 0, inner_lines - 1, :][:, None, :]
    chain_center = center[:, 0]
    chain_index = lax.broadcasted_iota(jnp.int32, (fields, groups, NX), 1)
    last_row = chain_index == groups - 1
    chain_mid = jnp.where(last_row, chain_center + 1.0 - tail_right, chain_center - tail_right - head_left)
    chain_low = jnp.where(chain_index > 0, -tail_left, 0.0)
    chain_up = jnp.where(last_row, 0.0, -head_right)
    separators, = cyclic_solve(chain_low, chain_mid, chain_up, (chain_side,))
    before = jnp.concatenate([jnp.zeros_like(separators[:, :1, :]), separators[:, :-1, :]], axis=1)
    interior = base_part + before[:, :, None, :] * left_spike + separators[:, :, None, :] * right_spike
    kept_values = jnp.concatenate([interior, separators[:, :, None, :]], axis=2).reshape(fields, NY // 2, NX)
    earlier_odd = jnp.concatenate([jnp.zeros_like(kept_values[:, :1, :]), kept_values[:, :-1, :]], axis=1)
    even_values = (even_lines + earlier_odd + kept_values) / factor
    merged = jnp.stack([even_values, kept_values], axis=2).reshape(fields, NY, NX)
    return jnp.einsum('fyk,ki->fiy', merged, transform, precision=HIGHEST)
```

```python
import functools
import math

import jax
import jax.numpy as jnp
import numpy as np
from jax import lax
from jax.experimental import pallas as pl
from jax.experimental.pallas import tpu as pltpu
from jax.sharding import PartitionSpec as P

LANES = 128
SEGMENTS = 8
TILE = 256
STEP = 32
GRID_AXES = ("gx", "gy")
MESH = pl.DeviceIdType.MESH


def mode_numbers(length):
    half = length // 2
    numbers = np.arange(half, dtype=np.int64) + 1
    return np.concatenate([2 * numbers, length + 1 - 2 * numbers])


def double_cosines(length):
    angles = mode_numbers(length).astype(np.float32) * np.float32(math.pi / (length + 1))
    return np.float32(2.0) * np.cos(angles.astype(np.float64)).astype(np.float32)


def constant_rows(length):
    half = length // 2
    columns = np.arange(half, dtype=np.int64)[None, :] + 1
    coarse = np.arange(half // STEP, dtype=np.int64)[:, None] * STEP
    fine = np.arange(STEP, dtype=np.int64)[:, None] + 1
    scale = math.sqrt(2.0 / (length + 1))
    angle = lambda rows: 2.0 * math.pi * (rows * columns % (length + 1)) / (length + 1)
    tables = (
        scale * np.sin(angle(coarse)),
        scale * np.cos(angle(coarse)),
        np.sin(angle(fine)),
        np.cos(angle(fine)),
        double_cosines(length).reshape(2, half),
        np.zeros((SEGMENTS - 2, half)),
    )
    return np.concatenate(tables).astype(np.float32)


def power(base, exponent):
    result = None
    while exponent:
        if exponent & 1:
            result = base if result is None else result * base
        exponent >>= 1
        if exponent:
            base = base * base
    return result


def decay_of(screening, cosines):
    factor = (4.0 + screening) - cosines
    excess = factor - 2.0
    root = jnp.sqrt(excess * (excess + 4.0))
    return 2.0 / (factor + root), root


def split(values):
    high = values.astype(jnp.bfloat16)
    return high, (values - high.astype(jnp.float32)).astype(jnp.bfloat16)


def mirrored(values):
    lanes = lax.broadcasted_iota(jnp.int32, values.shape, 1)
    return jnp.take_along_axis(values, LANES - 1 - lanes, axis=1)


def parity(shape):
    lanes = lax.broadcasted_iota(jnp.int32, shape, 1)
    return jnp.where(lanes % 2 == 0, 1.0, -1.0)


def tile_columns(t):
    return slice(t * TILE, (t + 1) * TILE)


def product(high, low, table_high, table_low):
    dot = functools.partial(jnp.dot, preferred_element_type=jnp.float32)
    return dot(high, table_high) + dot(low, table_high) + dot(high, table_low)


def peer(index):
    across = lax.axis_size("gy")
    return {"gx": index // across, "gy": index % across}


def boundary_states(groups, rows, moments_of, decay, root, left_parts, right_parts, left_states, right_states):
    position = lax.axis_index(GRID_AXES)
    stride = power(decay, rows // SEGMENTS)
    block = power(decay, rows)
    whole = power(decay, rows * groups + 1)
    moments = [moments_of((position + groups - d) % groups) for d in range(groups)]
    left_total = right_total = jnp.zeros_like(decay)
    for d in range(groups):
        left_total = block * left_total + moments[d][0:1, :]
        right_total = block * right_total + moments[groups - 1 - d][1:2, :]
    edge = -decay / (1.0 - whole * whole)
    left_state = edge * (right_total - whole * left_total)
    right_state = edge * (left_total - whole * right_total)
    left_own, right_own = left_state, right_state
    for d in range(groups):
        left_own = jnp.where(d == position, left_state, left_own)
        left_state = block * left_state + moments[d][0:1, :]
        e = groups - 1 - d
        right_own = jnp.where(e == position, right_state, right_own)
        right_state = block * right_state + moments[e][1:2, :]
    after_states = []
    for s in range(SEGMENTS):
        left_states[s : s + 1, :] = left_own
        left_own = stride * left_own + left_parts[s : s + 1, :]
        after_states.append(left_own)
    for s in reversed(range(SEGMENTS)):
        right_states[s : s + 1, :] = (right_own + decay * after_states[s]) / root
        right_own = stride * right_own + right_parts[s : s + 1, :]


def solve_lines(spectrum, decay, left_states, right_states, high, low):
    rows = spectrum.shape[0]
    steps = rows // SEGMENTS
    for h in range(2):
        columns = tile_columns(h)
        ratio = jnp.broadcast_to(decay[:, columns], (SEGMENTS, TILE))
        state = left_states[:, columns]
        sums = []
        for g in range(steps):
            state = ratio * state + spectrum[g * SEGMENTS : (g + 1) * SEGMENTS, columns]
            sums.append(state)
        state = right_states[:, columns]
        for g in reversed(range(0, steps, 2)):
            later = ratio * (state + sums[g + 1])
            state = ratio * (later + sums[g])
            place = pl.ds(h * rows + g * SEGMENTS, 2 * SEGMENTS)
            high[place, :], low[place, :] = split(jnp.concatenate([state, later], axis=0))


def line_sums(spectrum, decay, left_parts, right_parts):
    rows = spectrum.shape[0]
    steps = rows // SEGMENTS
    for h in range(2):
        columns = tile_columns(h)
        ratio = jnp.broadcast_to(decay[:, columns], (SEGMENTS, TILE))
        left = right = jnp.zeros((SEGMENTS, TILE), jnp.float32)
        for g in range(steps):
            mirror = steps - 1 - g
            left = ratio * left + spectrum[g * SEGMENTS : (g + 1) * SEGMENTS, columns]
            right = ratio * right + spectrum[mirror * SEGMENTS : (mirror + 1) * SEGMENTS, columns]
        left_parts[:, columns] = left
        right_parts[:, columns] = right


def forward_kernel(
    groups, pitch, source, screening, constants,
    table_high, table_low, partial, next_high, next_low,
    last_spectrum, last_left, last_right, last_moments, last_decay,
    rows_of, rows_sems, stage, arrived, high, low, back_high, back_low,
    spectrum, left_parts, right_parts, left_states, right_states,
    landed, send_sems, recv_sems,
):
    _, steps, length = source.shape
    rows = SEGMENTS * steps
    half = length // 2
    blocks = length // LANES
    tiles = half // TILE
    steps = rows // SEGMENTS
    last = tiles - 1
    position = lax.axis_index(GRID_AXES)

    rows_copies = [
        pltpu.make_async_copy(
            constants.at[:, pl.ds(t * TILE, TILE)], rows_of.at[:, pl.ds(t * TILE, TILE)], rows_sems.at[t]
        )
        for t in range(tiles)
    ]
    copies = [
        pltpu.make_async_copy(
            source.at[:, :, pl.ds(c * LANES, LANES)],
            stage.at[c].reshape(SEGMENTS, pitch, LANES).at[:, pl.ds(0, steps), :],
            arrived.at[c],
        )
        for c in range(blocks)
    ]
    rows_copies[0].start()
    for c in range(blocks // 2):
        copies[c].start()
        copies[blocks - 1 - c].start()
    for copy in rows_copies[1:]:
        copy.start()
    barrier = pltpu.get_barrier_semaphore()
    for d in range(1, groups):
        pl.semaphore_signal(barrier, inc=1, device_id=peer((position + d) % groups), device_id_type=MESH)

    def make_table(t):
        columns = tile_columns(t)
        fine_sin = rows_of[2 * coarse_rows : 2 * coarse_rows + STEP, columns]
        fine_cos = rows_of[2 * coarse_rows + STEP : 2 * coarse_rows + 2 * STEP, columns]
        for a in range(coarse_rows):
            values = rows_of[a : a + 1, columns] * fine_cos + rows_of[coarse_rows + a : coarse_rows + a + 1, columns] * fine_sin
            place = slice(a * STEP, (a + 1) * STEP)
            table_high[place, columns], table_low[place, columns] = split(values)

    coarse_rows = half // STEP
    cosine_row = 2 * coarse_rows + 2 * STEP

    def decay_tile(t):
        columns = tile_columns(t)
        cosines = [rows_of[cosine_row + h : cosine_row + h + 1, columns] for h in range(2)]
        return decay_of(screening[0], jnp.concatenate(cosines, axis=1))

    rows_copies[0].wait()
    make_table(0)
    signs = parity((2 * SEGMENTS, LANES))
    for c in range(blocks // 2):
        copies[c].wait()
        copies[blocks - 1 - c].wait()
        columns = pl.ds(c * LANES, LANES)
        for g in range(0, steps, 2):
            place = pl.ds(g * SEGMENTS, 2 * SEGMENTS)
            place_sum = pl.ds(rows + g * SEGMENTS, 2 * SEGMENTS)

            def load(column):
                pair = [stage[column, pl.ds(g + e, SEGMENTS, stride=pitch), :] for e in range(2)]
                return jnp.concatenate(pair, axis=0)

            near = load(c)
            far = mirrored(load(blocks - 1 - c))
            high[place, columns], low[place, columns] = split(near - far)
            high[place_sum, columns], low[place_sum, columns] = split((near + far) * signs)
    for copy in rows_copies[1:]:
        copy.wait()

    def lines_of(t):
        return last_spectrum if t == last else spectrum.at[t]

    def sums_of(t):
        return (last_left, last_right) if t == last else (left_parts.at[t], right_parts.at[t])

    sends = []
    for t in range(tiles):
        columns = tile_columns(t)
        values = product(high[...], low[...], table_high[:, columns], table_low[:, columns])
        if t + 1 < tiles:
            make_table(t + 1)
        lines_of(t)[:, :TILE] = values[:rows]
        lines_of(t)[:, TILE:] = values[rows:]
        decay, root = decay_tile(t)
        left_sums, right_sums = sums_of(t)
        line_sums(lines_of(t), decay, left_sums, right_sums)
        stride = power(decay, steps)
        left = right = jnp.zeros_like(decay)
        for s in range(SEGMENTS):
            left = stride * left + left_sums[s : s + 1, :]
            right = stride * right + right_sums[SEGMENTS - 1 - s : SEGMENTS - s, :]
        landed[t, 0, 0:1, :] = left
        landed[t, 0, 1:2, :] = right
        if t == 0:
            pl.semaphore_wait(barrier, groups - 1)
        for d in range(1, groups):
            send = pltpu.make_async_remote_copy(
                src_ref=landed.at[t, 0],
                dst_ref=landed.at[t, d],
                send_sem=send_sems.at[t, d],
                recv_sem=recv_sems.at[t, d],
                device_id=peer((position + d) % groups),
                device_id_type=MESH,
            )
            send.start()
            sends.append(send)
    last_decay[0:1, :], last_decay[1:2, :] = decay, root

    def receive(t):
        for send in sends[t * (groups - 1) : (t + 1) * (groups - 1)]:
            send.wait_recv()

    def multiply(t):
        inner = slice(t * TILE, (t + 1) * TILE)
        for n in range(tiles):
            columns = tile_columns(n)
            values = product(back_high[t], back_low[t], table_high[inner, columns], table_low[inner, columns])
            partial[:, columns] = values if t == 0 else partial[:, columns] + values

    if last < 2:
        partial[...] = jnp.zeros_like(partial)
    for t in range(last):
        receive(t)
        if t:
            multiply(t - 1)
        decay, root = decay_tile(t)
        boundary_states(
            groups, rows, lambda index, t=t: landed[t, index], decay, root,
            left_parts.at[t], right_parts.at[t], left_states.at[t], right_states.at[t],
        )
        target = (next_high, next_low) if t == last - 1 else (back_high.at[t], back_low.at[t])
        solve_lines(spectrum.at[t], decay, left_states.at[t], right_states.at[t], *target)
    receive(last)
    for d in range(groups):
        last_moments[d] = landed[last, d]
    for send in sends:
        send.wait_send()


def backward_kernel(
    groups, pitch, table_high, table_low, partial, next_high, next_low,
    last_spectrum, last_left, last_right, last_moments, last_decay,
    solved, acc, last_high, last_low, left_states, right_states, stage, stored,
):
    _, steps, length = solved.shape
    rows = SEGMENTS * steps
    half = length // 2
    blocks = length // LANES
    tiles = half // TILE
    steps = rows // SEGMENTS
    before = slice((tiles - 2) * TILE, (tiles - 1) * TILE)
    inner = slice((tiles - 1) * TILE, tiles * TILE)
    for n in range(tiles):
        columns = tile_columns(n)
        acc[:, columns] = partial[:, columns] + product(
            next_high[...], next_low[...], table_high[before, columns], table_low[before, columns]
        )
    decay, root = last_decay[0:1, :], last_decay[1:2, :]
    boundary_states(
        groups, rows, lambda index: last_moments[index], decay, root, last_left, last_right, left_states, right_states
    )
    solve_lines(last_spectrum, decay, left_states, right_states, last_high, last_low)
    signs = parity((SEGMENTS, LANES))
    copies = []
    for n in range(tiles):
        columns = tile_columns(n)
        values = acc[:, columns] + product(
            last_high[...], last_low[...], table_high[inner, columns], table_low[inner, columns]
        )
        for c in range(TILE // LANES):
            near = n * TILE // LANES + c
            far = blocks - 1 - near
            lanes = slice(c * LANES, (c + 1) * LANES)
            for g in range(steps):
                place = pl.ds(g, SEGMENTS, stride=pitch)
                odd = values[g * SEGMENTS : (g + 1) * SEGMENTS, lanes]
                even = values[rows + g * SEGMENTS : rows + (g + 1) * SEGMENTS, lanes] * signs
                stage[near, place, :] = even + odd
                stage[far, place, :] = mirrored(even - odd)
            for index in (near, far):
                copy = pltpu.make_async_copy(
                    stage.at[index].reshape(SEGMENTS, pitch, LANES).at[:, pl.ds(0, steps), :],
                    solved.at[:, :, pl.ds(index * LANES, LANES)],
                    stored.at[index],
                )
                copy.start()
                copies.append(copy)
    for copy in copies:
        copy.wait()


def on_device(source, screening):
    groups = lax.axis_size(GRID_AXES)
    fields, rows, length = source.shape
    half = length // 2
    tiles = half // TILE
    width = 2 * TILE
    steps = rows // SEGMENTS
    pitch = steps + 8 if steps % 16 == 0 else steps
    blocks = length // LANES
    constants = jnp.asarray(constant_rows(length))
    vmem = pl.BlockSpec(memory_space=pltpu.VMEM)
    smem = pl.BlockSpec(memory_space=pltpu.SMEM)
    hbm = pl.BlockSpec(memory_space=pl.ANY)
    f32 = lambda *shape: jax.ShapeDtypeStruct(shape, jnp.float32)
    bf16 = lambda *shape: jax.ShapeDtypeStruct(shape, jnp.bfloat16)
    stay = lambda array: pltpu.with_memory_space_constraint(array, pltpu.HBM)
    floats = lambda *shape: pltpu.VMEM(shape, jnp.float32)
    halves = lambda *shape: pltpu.VMEM(shape, jnp.bfloat16)
    staging = [floats(blocks, SEGMENTS * pitch, LANES), pltpu.SemaphoreType.DMA((blocks,))]

    def one_field(grid, constant):
        parts = pl.pallas_call(
            functools.partial(forward_kernel, groups, pitch),
            out_shape=[
                bf16(half, half), bf16(half, half), f32(2 * rows, half),
                bf16(2 * rows, TILE), bf16(2 * rows, TILE),
                f32(rows, width), f32(SEGMENTS, width), f32(SEGMENTS, width),
                f32(groups, 2, width), f32(2, width),
            ],
            in_specs=[hbm, smem, hbm],
            out_specs=[vmem] * 10,
            scratch_shapes=[floats(*constants.shape), pltpu.SemaphoreType.DMA((tiles,))]
            + staging
            + [halves(2 * rows, half)] * 2
            + [halves(tiles - 2, 2 * rows, TILE)] * 2
            + [floats(tiles - 1, rows, width)]
            + [floats(tiles - 1, SEGMENTS, width)] * 4
            + [floats(tiles, groups, 2, width)]
            + [pltpu.SemaphoreType.DMA((tiles, groups))] * 2,
            compiler_params=pltpu.CompilerParams(
                vmem_limit_bytes=40 * 2**20, collective_id=0, has_side_effects=True
            ),
            name="forward",
        )(stay(grid.reshape(SEGMENTS, steps, length)), constant, stay(constants))
        solved = pl.pallas_call(
            functools.partial(backward_kernel, groups, pitch),
            out_shape=f32(SEGMENTS, steps, length),
            in_specs=[vmem] * 10,
            out_specs=hbm,
            scratch_shapes=[floats(2 * rows, half)]
            + [halves(2 * rows, TILE)] * 2
            + [floats(SEGMENTS, width)] * 2
            + staging,
            compiler_params=pltpu.CompilerParams(vmem_limit_bytes=40 * 2**20),
            name="backward",
        )(*parts)
        return solved.reshape(rows, length)

    return jnp.stack([one_field(source[f], screening[f : f + 1]) for f in range(fields)])


def solution(mesh):
    return jax.shard_map(
        on_device,
        mesh=mesh,
        in_specs=(P("af", GRID_AXES, None), P("af")),
        out_specs=P("af", GRID_AXES, None),
        check_vma=False,
    )
```

```python
import functools
import math

import jax
import jax.numpy as jnp
import numpy as np
from jax import lax
from jax.experimental import pallas as pl
from jax.experimental.pallas import tpu as pltpu
from jax.sharding import PartitionSpec as P

LANES = 128
SEGMENTS = 8
TILE = 256
STEP = 32
COEFFICIENTS = 6
GRID_AXES = ("gx", "gy")
MESH = pl.DeviceIdType.MESH


def mode_numbers(length):
    half = length // 2
    numbers = np.arange(half, dtype=np.int64) + 1
    return np.concatenate([2 * numbers, length + 1 - 2 * numbers])


def double_cosines(length):
    angles = mode_numbers(length).astype(np.float32) * np.float32(math.pi / (length + 1))
    return np.float32(2.0) * np.cos(angles.astype(np.float64)).astype(np.float32)


def constant_rows(length):
    half = length // 2
    columns = np.arange(half, dtype=np.int64)[None, :] + 1
    coarse = np.arange(half // STEP, dtype=np.int64)[:, None] * STEP
    fine = np.arange(STEP, dtype=np.int64)[:, None] + 1
    scale = math.sqrt(2.0 / (length + 1))
    angle = lambda rows: 2.0 * math.pi * (rows * columns % (length + 1)) / (length + 1)
    tables = (
        scale * np.sin(angle(coarse)),
        scale * np.cos(angle(coarse)),
        np.sin(angle(fine)),
        np.cos(angle(fine)),
    )
    return np.concatenate(tables).astype(np.float32)


def cosine_rows(length):
    tiles = length // (2 * TILE)
    rows = double_cosines(length).reshape(2, tiles, TILE).transpose(1, 0, 2).reshape(tiles, 2 * TILE)
    return np.concatenate([rows, np.repeat(rows[-1:], -tiles % SEGMENTS, axis=0)])


def power(base, exponent):
    result = None
    while exponent:
        if exponent & 1:
            result = base if result is None else result * base
        exponent >>= 1
        if exponent:
            base = base * base
    return result


def decay_of(screening, cosines):
    factor = (4.0 + screening) - cosines
    excess = factor - 2.0
    root = jnp.sqrt(excess * (excess + 4.0))
    return 2.0 / (factor + root), root


def split(values):
    high = values.astype(jnp.bfloat16)
    return high, (values - high.astype(jnp.float32)).astype(jnp.bfloat16)


def mirrored(values):
    lanes = lax.broadcasted_iota(jnp.int32, values.shape, 1)
    return jnp.take_along_axis(values, LANES - 1 - lanes, axis=1)


def parity(shape):
    lanes = lax.broadcasted_iota(jnp.int32, shape, 1)
    return jnp.where(lanes % 2 == 0, 1.0, -1.0)


def tile_columns(t):
    return slice(t * TILE, (t + 1) * TILE)


def product(high, low, table_high, table_low):
    dot = functools.partial(jnp.dot, preferred_element_type=jnp.float32)
    return dot(high, table_high) + dot(low, table_high) + dot(high, table_low)


def peer(index):
    across = lax.axis_size("gy")
    return {"gx": index // across, "gy": index % across}


def store_coefficients(groups, rows, screening, cosines, coefficients):
    decay, root = decay_of(screening, cosines)
    whole = power(decay, rows * groups + 1)
    values = (
        decay,
        power(decay, rows // SEGMENTS),
        power(decay, rows),
        whole,
        -decay / (1.0 - whole * whole),
        1.0 / root,
    )
    for index, value in enumerate(values):
        coefficients[index] = value


def boundary_states(groups, moments_of, coefficients, left_parts, right_parts, left_states, right_states):
    decay, stride, block, whole, edge, scale = coefficients
    position = lax.axis_index(GRID_AXES)
    moments = [moments_of((position + groups - d) % groups) for d in range(groups)]
    left_total = right_total = jnp.zeros_like(decay)
    for d in range(groups):
        left_total = block * left_total + moments[d][0:1, :]
        right_total = block * right_total + moments[groups - 1 - d][1:2, :]
    left_state = edge * (right_total - whole * left_total)
    right_state = edge * (left_total - whole * right_total)
    left_own, right_own = left_state, right_state
    for d in range(groups):
        left_own = jnp.where(d == position, left_state, left_own)
        left_state = block * left_state + moments[d][0:1, :]
        e = groups - 1 - d
        right_own = jnp.where(e == position, right_state, right_own)
        right_state = block * right_state + moments[e][1:2, :]
    after_states = []
    for s in range(SEGMENTS):
        left_states[s : s + 1, :] = left_own
        left_own = stride * left_own + left_parts[s : s + 1, :]
        after_states.append(left_own)
    for s in reversed(range(SEGMENTS)):
        right_states[s : s + 1, :] = (right_own + decay * after_states[s]) * scale
        right_own = stride * right_own + right_parts[s : s + 1, :]


def solve_lines(spectrum, decay, left_states, right_states, high, low):
    rows = spectrum.shape[0]
    steps = rows // SEGMENTS
    for h in range(2):
        columns = tile_columns(h)
        ratio = jnp.broadcast_to(decay[:, columns], (SEGMENTS, TILE))
        state = left_states[:, columns]
        sums = []
        for g in range(steps):
            state = ratio * state + spectrum[g * SEGMENTS : (g + 1) * SEGMENTS, columns]
            sums.append(state)
        state = right_states[:, columns]
        for g in reversed(range(0, steps, 2)):
            later = ratio * (state + sums[g + 1])
            state = ratio * (later + sums[g])
            place = pl.ds(h * rows + g * SEGMENTS, 2 * SEGMENTS)
            high[place, :], low[place, :] = split(jnp.concatenate([state, later], axis=0))


def line_sums(spectrum, decay, stride, left_parts, right_parts, moments):
    rows = spectrum.shape[0]
    steps = rows // SEGMENTS
    for h in range(2):
        columns = tile_columns(h)
        ratio = jnp.broadcast_to(decay[:, columns], (SEGMENTS, TILE))
        left = right = jnp.zeros((SEGMENTS, TILE), jnp.float32)
        for g in range(steps):
            mirror = steps - 1 - g
            left = ratio * left + spectrum[g * SEGMENTS : (g + 1) * SEGMENTS, columns]
            right = ratio * right + spectrum[mirror * SEGMENTS : (mirror + 1) * SEGMENTS, columns]
        left_parts[:, columns] = left
        right_parts[:, columns] = right
    left = right = jnp.zeros_like(decay)
    for s in range(SEGMENTS):
        left = stride * left + left_parts[s : s + 1, :]
        right = stride * right + right_parts[SEGMENTS - 1 - s : SEGMENTS - s, :]
    moments[0:1, :] = left
    moments[1:2, :] = right


def forward_kernel(
    groups, pitch, source, screening, constants, cosines,
    table_high, table_low, partial, next_high, next_low,
    last_spectrum, last_left, last_right, last_moments, coefficients,
    angles, angle_sems, cosines_here, cosines_sem, stage, arrived, high, low, back_high, back_low,
    spectrum, left_parts, right_parts, left_states, right_states,
    landed, send_sems, recv_sems,
):
    _, steps, length = source.shape
    rows = SEGMENTS * steps
    half = length // 2
    blocks = length // LANES
    tiles = half // TILE
    last = tiles - 1
    position = lax.axis_index(GRID_AXES)

    angle_copies = [
        pltpu.make_async_copy(
            constants.at[:, pl.ds(t * TILE, TILE)], angles.at[:, pl.ds(t * TILE, TILE)], angle_sems.at[t]
        )
        for t in range(tiles)
    ]
    cosines_copy = pltpu.make_async_copy(cosines, cosines_here, cosines_sem.at[0])
    copies = [
        pltpu.make_async_copy(
            source.at[:, :, pl.ds(c * LANES, LANES)],
            stage.at[c].reshape(SEGMENTS, pitch, LANES).at[:, pl.ds(0, steps), :],
            arrived.at[c],
        )
        for c in range(blocks)
    ]
    angle_copies[0].start()
    cosines_copy.start()
    for c in range(blocks // 2):
        copies[c].start()
        copies[blocks - 1 - c].start()
    for copy in angle_copies[1:]:
        copy.start()
    barrier = pltpu.get_barrier_semaphore()
    for d in range(1, groups):
        pl.semaphore_signal(barrier, inc=1, device_id=peer((position + d) % groups), device_id_type=MESH)

    coarse_rows = half // STEP

    def make_table(t):
        columns = tile_columns(t)
        fine_sin = angles[2 * coarse_rows : 2 * coarse_rows + STEP, columns]
        fine_cos = angles[2 * coarse_rows + STEP : 2 * coarse_rows + 2 * STEP, columns]
        for a in range(coarse_rows):
            coarse_sin = angles[a : a + 1, columns]
            coarse_cos = angles[coarse_rows + a : coarse_rows + a + 1, columns]
            place = slice(a * STEP, (a + 1) * STEP)
            table_high[place, columns], table_low[place, columns] = split(coarse_sin * fine_cos + coarse_cos * fine_sin)

    def row_of(index, t):
        return coefficients[index, t : t + 1, :]

    angle_copies[0].wait()
    cosines_copy.wait()
    store_coefficients(groups, rows, screening[0], cosines_here[...], coefficients)
    make_table(0)
    signs = parity((2 * SEGMENTS, LANES))
    pairs = blocks // 2
    for begin in range(0, pairs, pairs // 2):
        chosen = range(begin, begin + pairs // 2)
        for c in chosen:
            copies[c].wait()
            copies[blocks - 1 - c].wait()
        for c in chosen:
            columns = pl.ds(c * LANES, LANES)
            for g in range(0, steps, 2):
                place = pl.ds(g * SEGMENTS, 2 * SEGMENTS)
                place_sum = pl.ds(rows + g * SEGMENTS, 2 * SEGMENTS)

                def load(column):
                    pair = [stage[column, pl.ds(g + e, SEGMENTS, stride=pitch), :] for e in range(2)]
                    return jnp.concatenate(pair, axis=0)

                near = load(c)
                far = mirrored(load(blocks - 1 - c))
                high[place, columns], low[place, columns] = split(near - far)
                high[place_sum, columns], low[place_sum, columns] = split((near + far) * signs)
    for copy in angle_copies[1:]:
        copy.wait()
    pl.semaphore_wait(barrier, groups - 1)

    def lines_of(t):
        return last_spectrum if t == last else spectrum.at[t]

    def sums_of(t):
        return (last_left, last_right) if t == last else (left_parts.at[t], right_parts.at[t])

    def transform(t, h):
        columns = tile_columns(t)
        for k in range(2):
            part = slice(k * rows // 2, (k + 1) * rows // 2)
            place = slice(h * rows + k * rows // 2, h * rows + (k + 1) * rows // 2)
            lines_of(t)[part, tile_columns(h)] = product(
                high[place, :], low[place, :], table_high[:, columns], table_low[:, columns]
            )

    sends = []

    def sum_lines(t):
        line_sums(lines_of(t), row_of(0, t), row_of(1, t), *sums_of(t), landed.at[t, 0])

    def send(t):
        for d in range(1, groups):
            copy = pltpu.make_async_remote_copy(
                src_ref=landed.at[t, 0],
                dst_ref=landed.at[t, d],
                send_sem=send_sems.at[t, d],
                recv_sem=recv_sems.at[t, d],
                device_id=peer((position + d) % groups),
                device_id_type=MESH,
            )
            copy.start()
            sends.append(copy)

    for t in range(tiles):
        transform(t, 0)
        if t:
            sum_lines(t - 1)
            send(t - 1)
        transform(t, 1)
        if t < last:
            make_table(t + 1)
    sum_lines(last)
    send(last)

    def receive(t):
        for copy in sends[t * (groups - 1) : (t + 1) * (groups - 1)]:
            copy.wait_recv()

    def multiply(t):
        inner = slice(t * TILE, (t + 1) * TILE)
        for n in range(tiles):
            columns = tile_columns(n)
            for h in range(2):
                place = slice(h * rows, (h + 1) * rows)
                values = product(
                    back_high[t, place, :], back_low[t, place, :], table_high[inner, columns], table_low[inner, columns]
                )
                partial[place, columns] = values if t == 0 else partial[place, columns] + values

    if last < 2:
        partial[...] = jnp.zeros_like(partial)
    for t in range(last):
        receive(t)
        if t:
            multiply(t - 1)
        boundary_states(
            groups, lambda index, t=t: landed[t, index], [row_of(i, t) for i in range(COEFFICIENTS)],
            left_parts.at[t], right_parts.at[t], left_states.at[t], right_states.at[t],
        )
        target = (next_high, next_low) if t == last - 1 else (back_high.at[t], back_low.at[t])
        solve_lines(spectrum.at[t], row_of(0, t), left_states.at[t], right_states.at[t], *target)
    receive(last)
    for d in range(groups):
        last_moments[d] = landed[last, d]
    for copy in sends:
        copy.wait_send()


def backward_kernel(
    groups, pitch, table_high, table_low, partial, next_high, next_low,
    last_spectrum, last_left, last_right, last_moments, coefficients,
    solved, acc, last_high, last_low, left_states, right_states, stage, stored,
):
    _, steps, length = solved.shape
    rows = SEGMENTS * steps
    half = length // 2
    blocks = length // LANES
    tiles = half // TILE
    before = slice((tiles - 2) * TILE, (tiles - 1) * TILE)
    inner = slice((tiles - 1) * TILE, tiles * TILE)

    def multiply(lines_high, lines_low, inner, n, base):
        columns = tile_columns(n)
        values = []
        for h in range(2):
            place = slice(h * rows, (h + 1) * rows)
            values.append(
                base[place, columns]
                + product(lines_high[place, :], lines_low[place, :], table_high[inner, columns], table_low[inner, columns])
            )
        return values

    for n in range(tiles):
        odd, even = multiply(next_high, next_low, before, n, partial)
        acc[:rows, tile_columns(n)] = odd
        acc[rows:, tile_columns(n)] = even
    row_values = [coefficients[i, tiles - 1 : tiles, :] for i in range(COEFFICIENTS)]
    boundary_states(
        groups, lambda index: last_moments[index], row_values, last_left, last_right, left_states, right_states
    )
    solve_lines(last_spectrum, row_values[0], left_states, right_states, last_high, last_low)
    signs = parity((SEGMENTS, LANES))
    copies = []
    later = multiply(last_high, last_low, inner, 0, acc)
    for n in range(tiles):
        odds, evens = later
        if n + 1 < tiles:
            later = multiply(last_high, last_low, inner, n + 1, acc)
        for c in range(TILE // LANES):
            near = n * TILE // LANES + c
            far = blocks - 1 - near
            lanes = slice(c * LANES, (c + 1) * LANES)
            for g in range(steps):
                place = pl.ds(g, SEGMENTS, stride=pitch)
                odd = odds[g * SEGMENTS : (g + 1) * SEGMENTS, lanes]
                even = evens[g * SEGMENTS : (g + 1) * SEGMENTS, lanes] * signs
                stage[near, place, :] = even + odd
                stage[far, place, :] = mirrored(even - odd)
        for c in range(TILE // LANES):
            near = n * TILE // LANES + c
            for index in (near, blocks - 1 - near):
                copy = pltpu.make_async_copy(
                    stage.at[index].reshape(SEGMENTS, pitch, LANES).at[:, pl.ds(0, steps), :],
                    solved.at[:, :, pl.ds(index * LANES, LANES)],
                    stored.at[index],
                )
                copy.start()
                copies.append(copy)
    for copy in copies:
        copy.wait()


def on_device(source, screening):
    groups = lax.axis_size(GRID_AXES)
    fields, rows, length = source.shape
    half = length // 2
    tiles = half // TILE
    width = 2 * TILE
    steps = rows // SEGMENTS
    pitch = steps + 8 if steps % 16 == 0 else steps
    blocks = length // LANES
    constants = jnp.asarray(constant_rows(length))
    cosines = jnp.asarray(cosine_rows(length))
    vmem = pl.BlockSpec(memory_space=pltpu.VMEM)
    hbm = pl.BlockSpec(memory_space=pl.ANY)
    f32 = lambda *shape: jax.ShapeDtypeStruct(shape, jnp.float32)
    bf16 = lambda *shape: jax.ShapeDtypeStruct(shape, jnp.bfloat16)
    stay = lambda array: pltpu.with_memory_space_constraint(array, pltpu.HBM)
    floats = lambda *shape: pltpu.VMEM(shape, jnp.float32)
    halves = lambda *shape: pltpu.VMEM(shape, jnp.bfloat16)
    staging = [floats(blocks, SEGMENTS * pitch, LANES), pltpu.SemaphoreType.DMA((blocks,))]

    def one_field(grid, constant):
        parts = pl.pallas_call(
            functools.partial(forward_kernel, groups, pitch),
            out_shape=[
                bf16(half, half), bf16(half, half), f32(2 * rows, half),
                bf16(2 * rows, TILE), bf16(2 * rows, TILE),
                f32(rows, width), f32(SEGMENTS, width), f32(SEGMENTS, width),
                f32(groups, 2, width), f32(COEFFICIENTS, *cosines.shape),
            ],
            in_specs=[hbm, pl.BlockSpec(memory_space=pltpu.SMEM), hbm, hbm],
            out_specs=[vmem] * 10,
            scratch_shapes=[
                floats(*constants.shape), pltpu.SemaphoreType.DMA((tiles,)),
                floats(*cosines.shape), pltpu.SemaphoreType.DMA((1,)),
            ]
            + staging
            + [halves(2 * rows, half)] * 2
            + [halves(tiles - 2, 2 * rows, TILE)] * 2
            + [floats(tiles - 1, rows, width)]
            + [floats(tiles - 1, SEGMENTS, width)] * 4
            + [floats(tiles, groups, 2, width)]
            + [pltpu.SemaphoreType.DMA((tiles, groups))] * 2,
            compiler_params=pltpu.CompilerParams(
                vmem_limit_bytes=40 * 2**20, collective_id=0, has_side_effects=True
            ),
            name="forward",
        )(stay(grid.reshape(SEGMENTS, steps, length)), constant, stay(constants), stay(cosines))
        solved = pl.pallas_call(
            functools.partial(backward_kernel, groups, pitch),
            out_shape=f32(SEGMENTS, steps, length),
            in_specs=[vmem] * 10,
            out_specs=hbm,
            scratch_shapes=[floats(2 * rows, half)]
            + [halves(2 * rows, TILE)] * 2
            + [floats(SEGMENTS, width)] * 2
            + staging,
            compiler_params=pltpu.CompilerParams(vmem_limit_bytes=40 * 2**20),
            name="backward",
        )(*parts)
        return solved.reshape(rows, length)

    return jnp.stack([one_field(source[f], screening[f : f + 1]) for f in range(fields)])


def solution(mesh):
    return jax.shard_map(
        on_device,
        mesh=mesh,
        in_specs=(P("af", GRID_AXES, None), P("af")),
        out_specs=P("af", GRID_AXES, None),
        check_vma=False,
    )
```

```python
import functools
import math

import jax
import jax.numpy as jnp
import numpy as np
from jax import lax
from jax.experimental import pallas as pl
from jax.experimental.pallas import tpu as pltpu
from jax.sharding import PartitionSpec as P

LANES = 128
SEGMENTS = 8
TILE = 256
STEP = 32
COEFFICIENTS = 6
GRID_AXES = ("gx", "gy")
MESH = pl.DeviceIdType.MESH


def mode_numbers(length):
    half = length // 2
    numbers = np.arange(half, dtype=np.int64) + 1
    return np.concatenate([2 * numbers, length + 1 - 2 * numbers])


def double_cosines(length):
    angles = mode_numbers(length).astype(np.float32) * np.float32(math.pi / (length + 1))
    return np.float32(2.0) * np.cos(angles.astype(np.float64)).astype(np.float32)


def constant_rows(length):
    half = length // 2
    columns = np.arange(half, dtype=np.int64)[None, :] + 1
    coarse = np.arange(half // STEP, dtype=np.int64)[:, None] * STEP
    fine = np.arange(STEP, dtype=np.int64)[:, None] + 1
    scale = math.sqrt(2.0 / (length + 1))
    angle = lambda rows: 2.0 * math.pi * (rows * columns % (length + 1)) / (length + 1)
    tables = (
        scale * np.sin(angle(coarse)),
        scale * np.cos(angle(coarse)),
        np.sin(angle(fine)),
        np.cos(angle(fine)),
    )
    return np.concatenate(tables).astype(np.float32)


def cosine_rows(length):
    tiles = length // (2 * TILE)
    rows = double_cosines(length).reshape(2, tiles, TILE).transpose(1, 0, 2).reshape(tiles, 2 * TILE)
    return np.concatenate([rows, np.repeat(rows[-1:], -tiles % SEGMENTS, axis=0)])


def power(base, exponent):
    result = None
    while exponent:
        if exponent & 1:
            result = base if result is None else result * base
        exponent >>= 1
        if exponent:
            base = base * base
    return result


def decay_of(screening, cosines):
    factor = (4.0 + screening) - cosines
    excess = factor - 2.0
    root = jnp.sqrt(excess * (excess + 4.0))
    return 2.0 / (factor + root), root


def split(values):
    high = values.astype(jnp.bfloat16)
    return high, (values - high.astype(jnp.float32)).astype(jnp.bfloat16)


def mirrored(values):
    lanes = lax.broadcasted_iota(jnp.int32, values.shape, 1)
    return jnp.take_along_axis(values, LANES - 1 - lanes, axis=1)


def parity(shape):
    lanes = lax.broadcasted_iota(jnp.int32, shape, 1)
    return jnp.where(lanes % 2 == 0, 1.0, -1.0)


def tile_columns(t):
    return slice(t * TILE, (t + 1) * TILE)


def product(high, low, table_high, table_low):
    dot = functools.partial(jnp.dot, preferred_element_type=jnp.float32)
    return dot(high, table_high) + dot(low, table_high) + dot(high, table_low)


def peer(index):
    across = lax.axis_size("gy")
    return {"gx": index // across, "gy": index % across}


def store_coefficients(groups, rows, screening, cosines, coefficients):
    decay, root = decay_of(screening, cosines)
    whole = power(decay, rows * groups + 1)
    values = (
        decay,
        power(decay, rows // SEGMENTS),
        power(decay, rows),
        whole,
        -decay / (1.0 - whole * whole),
        1.0 / root,
    )
    for index, value in enumerate(values):
        coefficients[index] = value


def boundary_states(groups, moments_of, coefficients, left_parts, right_parts, left_states, right_states, columns):
    decay, stride, block, whole, edge, scale = coefficients
    position = lax.axis_index(GRID_AXES)
    moments = [moments_of((position + groups - d) % groups) for d in range(groups)]
    left_total = right_total = jnp.zeros_like(decay)
    for d in range(groups):
        left_total = block * left_total + moments[d][0:1, :]
        right_total = block * right_total + moments[groups - 1 - d][1:2, :]
    left_state = edge * (right_total - whole * left_total)
    right_state = edge * (left_total - whole * right_total)
    left_own, right_own = left_state, right_state
    for d in range(groups):
        left_own = jnp.where(d == position, left_state, left_own)
        left_state = block * left_state + moments[d][0:1, :]
        e = groups - 1 - d
        right_own = jnp.where(e == position, right_state, right_own)
        right_state = block * right_state + moments[e][1:2, :]
    after_states = []
    for s in range(SEGMENTS):
        left_states[s : s + 1, columns] = left_own
        left_own = stride * left_own + left_parts[s : s + 1, columns]
        after_states.append(left_own)
    for s in reversed(range(SEGMENTS)):
        right_states[s : s + 1, columns] = (right_own + decay * after_states[s]) * scale
        right_own = stride * right_own + right_parts[s : s + 1, columns]


def solve_lines(spectrum, decay, left_states, right_states, high, low, parts=(0, 1)):
    rows = spectrum.shape[0]
    steps = rows // SEGMENTS
    for h in parts:
        columns = tile_columns(h)
        ratio = jnp.broadcast_to(decay[:, columns], (SEGMENTS, TILE))
        state = left_states[:, columns]
        sums = []
        for g in range(steps):
            state = ratio * state + spectrum[g * SEGMENTS : (g + 1) * SEGMENTS, columns]
            sums.append(state)
        state = right_states[:, columns]
        for g in reversed(range(0, steps, 2)):
            later = ratio * (state + sums[g + 1])
            state = ratio * (later + sums[g])
            place = pl.ds((h - parts[0]) * rows + g * SEGMENTS, 2 * SEGMENTS)
            high[place, :], low[place, :] = split(jnp.concatenate([state, later], axis=0))


def line_sums(spectrum, decay, stride, left_parts, right_parts, moments, parts=(0, 1)):
    rows = spectrum.shape[0]
    steps = rows // SEGMENTS
    for h in parts:
        columns = tile_columns(h)
        ratio = jnp.broadcast_to(decay[:, columns], (SEGMENTS, TILE))
        left = right = jnp.zeros((SEGMENTS, TILE), jnp.float32)
        for g in range(steps):
            mirror = steps - 1 - g
            left = ratio * left + spectrum[g * SEGMENTS : (g + 1) * SEGMENTS, columns]
            right = ratio * right + spectrum[mirror * SEGMENTS : (mirror + 1) * SEGMENTS, columns]
        left_parts[:, columns] = left
        right_parts[:, columns] = right
        jump = stride[:, columns]
        left = right = jnp.zeros_like(jump)
        for s in range(SEGMENTS):
            left = jump * left + left_parts[s : s + 1, columns]
            right = jump * right + right_parts[SEGMENTS - 1 - s : SEGMENTS - s, columns]
        moments[0:1, columns] = left
        moments[1:2, columns] = right


def forward_kernel(
    groups, pitch, source, screening, constants, cosines,
    table_high, table_low, partial, next_high, next_low,
    last_spectrum, last_left, last_right, last_moments, coefficients,
    angles, angle_sems, cosines_here, cosines_sem, stage, arrived, high, low, back_high, back_low,
    spectrum, left_parts, right_parts, left_states, right_states, last_left_states, last_right_states,
    landed, send_sems, recv_sems,
):
    _, steps, length = source.shape
    rows = SEGMENTS * steps
    half = length // 2
    blocks = length // LANES
    tiles = half // TILE
    last = tiles - 1
    position = lax.axis_index(GRID_AXES)

    angle_copies = [
        pltpu.make_async_copy(
            constants.at[:, pl.ds(t * TILE, TILE)], angles.at[:, pl.ds(t * TILE, TILE)], angle_sems.at[t]
        )
        for t in range(tiles)
    ]
    cosines_copy = pltpu.make_async_copy(cosines, cosines_here, cosines_sem.at[0])
    copies = [
        pltpu.make_async_copy(
            source.at[:, :, pl.ds(c * LANES, LANES)],
            stage.at[c].reshape(SEGMENTS, pitch, LANES).at[:, pl.ds(0, steps), :],
            arrived.at[c],
        )
        for c in range(blocks)
    ]
    angle_copies[0].start()
    cosines_copy.start()
    for c in range(blocks // 2):
        copies[c].start()
        copies[blocks - 1 - c].start()
    for copy in angle_copies[1:]:
        copy.start()
    barrier = pltpu.get_barrier_semaphore()
    for d in range(1, groups):
        pl.semaphore_signal(barrier, inc=1, device_id=peer((position + d) % groups), device_id_type=MESH)

    coarse_rows = half // STEP

    def make_table(t):
        columns = tile_columns(t)
        fine_sin = angles[2 * coarse_rows : 2 * coarse_rows + STEP, columns]
        fine_cos = angles[2 * coarse_rows + STEP : 2 * coarse_rows + 2 * STEP, columns]
        for a in range(coarse_rows):
            coarse_sin = angles[a : a + 1, columns]
            coarse_cos = angles[coarse_rows + a : coarse_rows + a + 1, columns]
            place = slice(a * STEP, (a + 1) * STEP)
            table_high[place, columns], table_low[place, columns] = split(coarse_sin * fine_cos + coarse_cos * fine_sin)

    def row_of(index, t):
        return coefficients[index, t : t + 1, :]

    angle_copies[0].wait()
    cosines_copy.wait()
    store_coefficients(groups, rows, screening[0], cosines_here[...], coefficients)
    make_table(0)
    signs = parity((2 * SEGMENTS, LANES))
    pairs = blocks // 2
    for begin in range(0, pairs, pairs // 2):
        chosen = range(begin, begin + pairs // 2)
        for c in chosen:
            copies[c].wait()
            copies[blocks - 1 - c].wait()
        if begin:
            for copy in angle_copies[1:]:
                copy.wait()
            pl.semaphore_wait(barrier, groups - 1)
        for c in chosen:
            columns = pl.ds(c * LANES, LANES)
            for g in range(0, steps, 2):
                place = pl.ds(g * SEGMENTS, 2 * SEGMENTS)
                place_sum = pl.ds(rows + g * SEGMENTS, 2 * SEGMENTS)

                def load(column):
                    pair = [stage[column, pl.ds(g + e, SEGMENTS, stride=pitch), :] for e in range(2)]
                    return jnp.concatenate(pair, axis=0)

                near = load(c)
                far = mirrored(load(blocks - 1 - c))
                high[place, columns], low[place, columns] = split(near - far)
                high[place_sum, columns], low[place_sum, columns] = split((near + far) * signs)
    def lines_of(t):
        return last_spectrum if t == last else spectrum.at[t]

    def sums_of(t):
        return (last_left, last_right) if t == last else (left_parts.at[t], right_parts.at[t])

    def transform(t, h):
        columns = tile_columns(t)
        for k in range(2):
            part = slice(k * rows // 2, (k + 1) * rows // 2)
            place = slice(h * rows + k * rows // 2, h * rows + (k + 1) * rows // 2)
            lines_of(t)[part, tile_columns(h)] = product(
                high[place, :], low[place, :], table_high[:, columns], table_low[:, columns]
            )

    every = (0, 1)
    whole_tile = slice(0, 2 * TILE)
    parcels = [(t, every, whole_tile) for t in range(last)] + [(last, (h,), tile_columns(h)) for h in every]

    def sum_lines(t, parts=every):
        line_sums(lines_of(t), row_of(0, t), row_of(1, t), *sums_of(t), landed.at[t, 0], parts)

    def send(p):
        t, _, columns = parcels[p]
        for d in range(1, groups):
            pltpu.make_async_remote_copy(
                src_ref=landed.at[t, 0, :, columns],
                dst_ref=landed.at[t, d, :, columns],
                send_sem=send_sems.at[p],
                recv_sem=recv_sems.at[p],
                device_id=peer((position + d) % groups),
                device_id_type=MESH,
            ).start()

    def all_of(p):
        t, _, columns = parcels[p]
        ref = landed.at[t, pl.ds(1, groups - 1), :, columns]
        return pltpu.make_async_remote_copy(
            src_ref=ref,
            dst_ref=ref,
            send_sem=send_sems.at[p],
            recv_sem=recv_sems.at[p],
            device_id=peer((position + 1) % groups),
            device_id_type=MESH,
        )

    for t in range(tiles):
        transform(t, 0)
        if t:
            sum_lines(t - 1)
            send(t - 1)
        transform(t, 1)
        if t < last:
            make_table(t + 1)
    sum_lines(last, (0,))
    send(last)
    sum_lines(last, (1,))
    send(tiles)

    def multiply(t):
        inner = slice(t * TILE, (t + 1) * TILE)
        for n in range(tiles):
            columns = tile_columns(n)
            for h in range(2):
                place = slice(h * rows, (h + 1) * rows)
                values = product(
                    back_high[t, place, :], back_low[t, place, :], table_high[inner, columns], table_low[inner, columns]
                )
                partial[place, columns] = values if t == 0 else partial[place, columns] + values

    for p in range(tiles):
        t, parts, columns = parcels[p]
        all_of(p).wait_recv()
        if p:
            multiply(p - 1)
        states = (last_left_states, last_right_states) if t == last else (left_states.at[t], right_states.at[t])
        boundary_states(
            groups, lambda index: landed[t, index, :, columns], [row_of(i, t)[:, columns] for i in range(COEFFICIENTS)],
            *sums_of(t), *states, columns,
        )
        target = (next_high, next_low) if t == last else (back_high.at[t], back_low.at[t])
        solve_lines(lines_of(t), row_of(0, t), *states, *target, parts)
    all_of(tiles).wait_recv()
    for d in range(groups):
        last_moments[d] = landed[last, d]
    for p in range(tiles + 1):
        all_of(p).wait_send()


def backward_kernel(
    groups, pitch, table_high, table_low, partial, next_high, next_low,
    last_spectrum, last_left, last_right, last_moments, coefficients,
    solved, acc, last_high, last_low, left_states, right_states, stage, stored,
):
    _, steps, length = solved.shape
    rows = SEGMENTS * steps
    half = length // 2
    blocks = length // LANES
    tiles = half // TILE
    inner = slice((tiles - 1) * TILE, tiles * TILE)

    def multiply(lines_high, lines_low, h, n):
        columns = tile_columns(n)
        values = []
        for k in range(2):
            part = slice(k * rows // 2, (k + 1) * rows // 2)
            place = slice(h * rows + k * rows // 2, h * rows + (k + 1) * rows // 2)
            values.append(
                partial[place, columns]
                + product(lines_high[part, :], lines_low[part, :], table_high[inner, columns], table_low[inner, columns])
            )
        return jnp.concatenate(values, axis=0)

    for n in range(tiles):
        acc[:, tile_columns(n)] = multiply(next_high, next_low, 0, n)
    columns = tile_columns(1)
    row_values = [coefficients[i, tiles - 1 : tiles, columns] for i in range(COEFFICIENTS)]
    boundary_states(
        groups, lambda index: last_moments[index, :, columns], row_values,
        last_left, last_right, left_states, right_states, columns,
    )
    solve_lines(
        last_spectrum, coefficients[0, tiles - 1 : tiles, :], left_states, right_states, last_high, last_low, (1,)
    )
    signs = parity((SEGMENTS, LANES))
    copies = []
    later = multiply(last_high, last_low, 1, 0)
    for n in range(tiles):
        evens = later
        if n + 1 < tiles:
            later = multiply(last_high, last_low, 1, n + 1)
        for c in range(TILE // LANES):
            near = n * TILE // LANES + c
            far = blocks - 1 - near
            lanes = slice(c * LANES, (c + 1) * LANES)
            for g in range(steps):
                place = pl.ds(g, SEGMENTS, stride=pitch)
                odd = acc[g * SEGMENTS : (g + 1) * SEGMENTS, near * LANES : (near + 1) * LANES]
                even = evens[g * SEGMENTS : (g + 1) * SEGMENTS, lanes] * signs
                stage[near, place, :] = even + odd
                stage[far, place, :] = mirrored(even - odd)
        for c in range(TILE // LANES):
            near = n * TILE // LANES + c
            for index in (near, blocks - 1 - near):
                copy = pltpu.make_async_copy(
                    stage.at[index].reshape(SEGMENTS, pitch, LANES).at[:, pl.ds(0, steps), :],
                    solved.at[:, :, pl.ds(index * LANES, LANES)],
                    stored.at[index],
                )
                copy.start()
                copies.append(copy)
    for copy in copies:
        copy.wait()


def on_device(source, screening):
    groups = lax.axis_size(GRID_AXES)
    fields, rows, length = source.shape
    half = length // 2
    tiles = half // TILE
    width = 2 * TILE
    steps = rows // SEGMENTS
    pitch = steps + 8 if steps % 16 == 0 else steps
    blocks = length // LANES
    constants = jnp.asarray(constant_rows(length))
    cosines = jnp.asarray(cosine_rows(length))
    vmem = pl.BlockSpec(memory_space=pltpu.VMEM)
    hbm = pl.BlockSpec(memory_space=pl.ANY)
    f32 = lambda *shape: jax.ShapeDtypeStruct(shape, jnp.float32)
    bf16 = lambda *shape: jax.ShapeDtypeStruct(shape, jnp.bfloat16)
    stay = lambda array: pltpu.with_memory_space_constraint(array, pltpu.HBM)
    floats = lambda *shape: pltpu.VMEM(shape, jnp.float32)
    halves = lambda *shape: pltpu.VMEM(shape, jnp.bfloat16)
    staging = [floats(blocks, SEGMENTS * pitch, LANES), pltpu.SemaphoreType.DMA((blocks,))]

    def one_field(grid, constant):
        parts = pl.pallas_call(
            functools.partial(forward_kernel, groups, pitch),
            out_shape=[
                bf16(half, half), bf16(half, half), f32(2 * rows, half),
                bf16(rows, TILE), bf16(rows, TILE),
                f32(rows, width), f32(SEGMENTS, width), f32(SEGMENTS, width),
                f32(groups, 2, width), f32(COEFFICIENTS, *cosines.shape),
            ],
            in_specs=[hbm, pl.BlockSpec(memory_space=pltpu.SMEM), hbm, hbm],
            out_specs=[vmem] * 10,
            scratch_shapes=[
                floats(*constants.shape), pltpu.SemaphoreType.DMA((tiles,)),
                floats(*cosines.shape), pltpu.SemaphoreType.DMA((1,)),
            ]
            + staging
            + [halves(2 * rows, half)] * 2
            + [halves(tiles - 1, 2 * rows, TILE)] * 2
            + [floats(tiles - 1, rows, width)]
            + [floats(tiles - 1, SEGMENTS, width)] * 4
            + [floats(SEGMENTS, width)] * 2
            + [floats(tiles, groups, 2, width)]
            + [pltpu.SemaphoreType.DMA((tiles + 1,))] * 2,
            compiler_params=pltpu.CompilerParams(
                vmem_limit_bytes=40 * 2**20, collective_id=0, has_side_effects=True
            ),
            name="forward",
        )(stay(grid.reshape(SEGMENTS, steps, length)), constant, stay(constants), stay(cosines))
        solved = pl.pallas_call(
            functools.partial(backward_kernel, groups, pitch),
            out_shape=f32(SEGMENTS, steps, length),
            in_specs=[vmem] * 10,
            out_specs=hbm,
            scratch_shapes=[floats(rows, half)]
            + [halves(rows, TILE)] * 2
            + [floats(SEGMENTS, width)] * 2
            + staging,
            compiler_params=pltpu.CompilerParams(vmem_limit_bytes=40 * 2**20),
            name="backward",
        )(*parts)
        return solved.reshape(rows, length)

    return jnp.stack([one_field(source[f], screening[f : f + 1]) for f in range(fields)])


def solution(mesh):
    return jax.shard_map(
        on_device,
        mesh=mesh,
        in_specs=(P("af", GRID_AXES, None), P("af")),
        out_specs=P("af", GRID_AXES, None),
        check_vma=False,
    )
```

```python
import functools
import math

import jax
import jax.numpy as jnp
import numpy as np
from jax import lax
from jax.experimental import pallas as pl
from jax.experimental.pallas import tpu as pltpu
from jax.sharding import PartitionSpec as P

LANES = 128
SEGMENTS = 8
TILE = 256
STEP = 32
COEFFICIENTS = 6
AHEAD = 2
GRID_AXES = ("gx", "gy")
MESH = pl.DeviceIdType.MESH


def mode_numbers(length):
    half = length // 2
    numbers = np.arange(half, dtype=np.int64) + 1
    return np.concatenate([2 * numbers, length + 1 - 2 * numbers])


def double_cosines(length):
    angles = mode_numbers(length).astype(np.float32) * np.float32(math.pi / (length + 1))
    return np.float32(2.0) * np.cos(angles.astype(np.float64)).astype(np.float32)


def constant_rows(length):
    half = length // 2
    columns = np.arange(half, dtype=np.int64)[None, :] + 1
    coarse = np.arange(half // STEP, dtype=np.int64)[:, None] * STEP
    fine = np.arange(STEP, dtype=np.int64)[:, None] + 1
    scale = math.sqrt(2.0 / (length + 1))
    angle = lambda rows: 2.0 * math.pi * (rows * columns % (length + 1)) / (length + 1)
    tables = (
        scale * np.sin(angle(coarse)),
        scale * np.cos(angle(coarse)),
        np.sin(angle(fine)),
        np.cos(angle(fine)),
    )
    return np.concatenate(tables).astype(np.float32)


def cosine_rows(length):
    tiles = length // (2 * TILE)
    rows = double_cosines(length).reshape(2, tiles, TILE).transpose(1, 0, 2).reshape(tiles, 2 * TILE)
    return np.concatenate([rows, np.repeat(rows[-1:], -tiles % SEGMENTS, axis=0)])


def power(base, exponent):
    result = None
    while exponent:
        if exponent & 1:
            result = base if result is None else result * base
        exponent >>= 1
        if exponent:
            base = base * base
    return result


def decay_of(screening, cosines):
    factor = (4.0 + screening) - cosines
    excess = factor - 2.0
    root = jnp.sqrt(excess * (excess + 4.0))
    return 2.0 / (factor + root), root


def split(values):
    high = values.astype(jnp.bfloat16)
    return high, (values - high.astype(jnp.float32)).astype(jnp.bfloat16)


def mirrored(values):
    lanes = lax.broadcasted_iota(jnp.int32, values.shape, 1)
    return jnp.take_along_axis(values, LANES - 1 - lanes, axis=1)


def parity(shape):
    lanes = lax.broadcasted_iota(jnp.int32, shape, 1)
    return jnp.where(lanes % 2 == 0, 1.0, -1.0)


def tile_columns(t):
    return slice(t * TILE, (t + 1) * TILE)


def product(high, low, table_high, table_low):
    dot = functools.partial(jnp.dot, preferred_element_type=jnp.float32)
    return dot(high, table_high) + dot(low, table_high) + dot(high, table_low)


def peer(index):
    across = lax.axis_size("gy")
    return {"gx": index // across, "gy": index % across}


def store_coefficients(groups, rows, screening, cosines, coefficients):
    decay, root = decay_of(screening, cosines)
    whole = power(decay, rows * groups + 1)
    values = (
        decay,
        power(decay, rows // SEGMENTS),
        power(decay, rows),
        whole,
        -decay / (1.0 - whole * whole),
        1.0 / root,
    )
    for index, value in enumerate(values):
        coefficients[index] = value


def boundary_states(groups, moments_of, coefficients, left_parts, right_parts, left_states, right_states, columns):
    decay, stride, block, whole, edge, scale = coefficients
    position = lax.axis_index(GRID_AXES)
    moments = [moments_of((position + groups - d) % groups) for d in range(groups)]
    left_total = right_total = jnp.zeros_like(decay)
    for d in range(groups):
        left_total = block * left_total + moments[d][0:1, :]
        right_total = block * right_total + moments[groups - 1 - d][1:2, :]
    left_state = edge * (right_total - whole * left_total)
    right_state = edge * (left_total - whole * right_total)
    left_own, right_own = left_state, right_state
    for d in range(groups):
        left_own = jnp.where(d == position, left_state, left_own)
        left_state = block * left_state + moments[d][0:1, :]
        e = groups - 1 - d
        right_own = jnp.where(e == position, right_state, right_own)
        right_state = block * right_state + moments[e][1:2, :]
    after_states = []
    for s in range(SEGMENTS):
        left_states[s : s + 1, columns] = left_own
        left_own = stride * left_own + left_parts[s : s + 1, columns]
        after_states.append(left_own)
    for s in reversed(range(SEGMENTS)):
        right_states[s : s + 1, columns] = (right_own + decay * after_states[s]) * scale
        right_own = stride * right_own + right_parts[s : s + 1, columns]


def solve_lines(spectrum, decay, left_states, right_states, high, low, parts=(0, 1)):
    rows = spectrum.shape[0]
    steps = rows // SEGMENTS
    for h in parts:
        columns = tile_columns(h)
        ratio = jnp.broadcast_to(decay[:, columns], (SEGMENTS, TILE))
        state = left_states[:, columns]
        sums = []
        for g in range(steps):
            state = ratio * state + spectrum[g * SEGMENTS : (g + 1) * SEGMENTS, columns]
            sums.append(state)
        state = right_states[:, columns]
        for g in reversed(range(0, steps, 2)):
            later = ratio * (state + sums[g + 1])
            state = ratio * (later + sums[g])
            place = pl.ds((h - parts[0]) * rows + g * SEGMENTS, 2 * SEGMENTS)
            high[place, :], low[place, :] = split(jnp.concatenate([state, later], axis=0))


def line_sums(spectrum, decay, stride, left_parts, right_parts, moments, parts=(0, 1)):
    rows = spectrum.shape[0]
    steps = rows // SEGMENTS
    for h in parts:
        columns = tile_columns(h)
        ratio = jnp.broadcast_to(decay[:, columns], (SEGMENTS, TILE))
        left = right = jnp.zeros((SEGMENTS, TILE), jnp.float32)
        for g in range(steps):
            mirror = steps - 1 - g
            left = ratio * left + spectrum[g * SEGMENTS : (g + 1) * SEGMENTS, columns]
            right = ratio * right + spectrum[mirror * SEGMENTS : (mirror + 1) * SEGMENTS, columns]
        left_parts[:, columns] = left
        right_parts[:, columns] = right
        jump = stride[:, columns]
        left = right = jnp.zeros_like(jump)
        for s in range(SEGMENTS):
            left = jump * left + left_parts[s : s + 1, columns]
            right = jump * right + right_parts[SEGMENTS - 1 - s : SEGMENTS - s, columns]
        moments[0:1, columns] = left
        moments[1:2, columns] = right


def forward_kernel(
    groups, pitch, early, source, screening, constants, cosines,
    table_high, table_low, partial, next_high, next_low,
    last_spectrum, last_left, last_right, last_moments, coefficients,
    angles, angle_sems, cosines_here, cosines_sem, stage, arrived, high, low, back_high, back_low,
    spectrum, left_parts, right_parts, left_states, right_states,
    landed, send_sems, recv_sems,
):
    _, steps, length = source.shape
    rows = SEGMENTS * steps
    half = length // 2
    blocks = length // LANES
    tiles = half // TILE
    last = tiles - 1
    position = lax.axis_index(GRID_AXES)

    angle_copies = [
        pltpu.make_async_copy(
            constants.at[:, pl.ds(t * TILE, TILE)], angles.at[:, pl.ds(t * TILE, TILE)], angle_sems.at[t]
        )
        for t in range(tiles)
    ]
    cosines_copy = pltpu.make_async_copy(cosines, cosines_here, cosines_sem.at[0])
    copies = [
        pltpu.make_async_copy(
            source.at[:, :, pl.ds(c * LANES, LANES)],
            stage.at[c].reshape(SEGMENTS, pitch, LANES).at[:, pl.ds(0, steps), :],
            arrived.at[c],
        )
        for c in range(blocks)
    ]
    angle_copies[0].start()
    cosines_copy.start()
    for c in range(blocks // 2):
        copies[c].start()
        copies[blocks - 1 - c].start()
    for copy in angle_copies[1:]:
        copy.start()
    barrier = pltpu.get_barrier_semaphore()
    for d in range(1, groups):
        pl.semaphore_signal(barrier, inc=1, device_id=peer((position + d) % groups), device_id_type=MESH)

    coarse_rows = half // STEP

    def make_table(t):
        columns = tile_columns(t)
        fine_sin = angles[2 * coarse_rows : 2 * coarse_rows + STEP, columns]
        fine_cos = angles[2 * coarse_rows + STEP : 2 * coarse_rows + 2 * STEP, columns]
        for a in range(coarse_rows):
            coarse_sin = angles[a : a + 1, columns]
            coarse_cos = angles[coarse_rows + a : coarse_rows + a + 1, columns]
            place = slice(a * STEP, (a + 1) * STEP)
            table_high[place, columns], table_low[place, columns] = split(coarse_sin * fine_cos + coarse_cos * fine_sin)

    def row_of(index, t):
        return coefficients[index, t : t + 1, :]

    angle_copies[0].wait()
    cosines_copy.wait()
    store_coefficients(groups, rows, screening[0], cosines_here[...], coefficients)
    make_table(0)
    signs = parity((2 * SEGMENTS, LANES))
    pairs = blocks // 2
    for begin in range(0, pairs, pairs // 2):
        chosen = range(begin, begin + pairs // 2)
        for c in chosen:
            copies[c].wait()
            copies[blocks - 1 - c].wait()
        if begin:
            for copy in angle_copies[1:]:
                copy.wait()
            pl.semaphore_wait(barrier, groups - 1)
        for c in chosen:
            columns = pl.ds(c * LANES, LANES)
            for g in range(0, steps, 2):
                place = pl.ds(g * SEGMENTS, 2 * SEGMENTS)
                place_sum = pl.ds(rows + g * SEGMENTS, 2 * SEGMENTS)

                def load(column):
                    pair = [stage[column, pl.ds(g + e, SEGMENTS, stride=pitch), :] for e in range(2)]
                    return jnp.concatenate(pair, axis=0)

                near = load(c)
                far = mirrored(load(blocks - 1 - c))
                high[place, columns], low[place, columns] = split(near - far)
                high[place_sum, columns], low[place_sum, columns] = split((near + far) * signs)
    def lines_of(t):
        return last_spectrum if t == last else spectrum.at[t]

    def sums_of(t):
        return (last_left, last_right) if t == last else (left_parts.at[t], right_parts.at[t])

    def transform(t, h):
        columns = tile_columns(t)
        for k in range(2):
            part = slice(k * rows // 2, (k + 1) * rows // 2)
            place = slice(h * rows + k * rows // 2, h * rows + (k + 1) * rows // 2)
            lines_of(t)[part, tile_columns(h)] = product(
                high[place, :], low[place, :], table_high[:, columns], table_low[:, columns]
            )

    every = (0, 1)
    whole_tile = slice(0, 2 * TILE)
    parcels = [(t, every, whole_tile) for t in range(last)] + [(last, (h,), tile_columns(h)) for h in every]

    def sum_lines(t, parts=every):
        line_sums(lines_of(t), row_of(0, t), row_of(1, t), *sums_of(t), landed.at[t, 0], parts)

    def send(p):
        t, _, columns = parcels[p]
        for d in range(1, groups):
            pltpu.make_async_remote_copy(
                src_ref=landed.at[t, 0, :, columns],
                dst_ref=landed.at[t, d, :, columns],
                send_sem=send_sems.at[p],
                recv_sem=recv_sems.at[p],
                device_id=peer((position + d) % groups),
                device_id_type=MESH,
            ).start()

    def all_of(p):
        t, _, columns = parcels[p]
        ref = landed.at[t, pl.ds(1, groups - 1), :, columns]
        return pltpu.make_async_remote_copy(
            src_ref=ref,
            dst_ref=ref,
            send_sem=send_sems.at[p],
            recv_sem=recv_sems.at[p],
            device_id=peer((position + 1) % groups),
            device_id_type=MESH,
        )

    for t in range(tiles):
        transform(t, 0)
        if t:
            sum_lines(t - 1)
            send(t - 1)
        transform(t, 1)
        if t < last:
            make_table(t + 1)
    sum_lines(last, (0,))
    send(last)
    sum_lines(last, (1,))
    send(tiles)

    def multiply(t, high, low, chosen):
        inner = slice(t * TILE, (t + 1) * TILE)
        for n in chosen:
            columns = tile_columns(n)
            for h in every:
                place = slice(h * rows, (h + 1) * rows)
                values = product(high[place, :], low[place, :], table_high[inner, columns], table_low[inner, columns])
                partial[place, columns] = values if t == 0 else partial[place, columns] + values

    for t in range(last):
        all_of(t).wait_recv()
        boundary_states(
            groups, lambda index: landed[t, index], [row_of(i, t) for i in range(COEFFICIENTS)],
            *sums_of(t), left_states.at[t], right_states.at[t], whole_tile,
        )
        target = (next_high, next_low) if t == last - 1 else (back_high.at[t], back_low.at[t])
        solve_lines(lines_of(t), row_of(0, t), left_states.at[t], right_states.at[t], *target)
        multiply(t, *target, range(early if t == last - 1 else tiles))
    all_of(last).wait_recv()
    all_of(tiles).wait_recv()
    for d in range(groups):
        last_moments[d] = landed[last, d]
    for p in range(tiles + 1):
        all_of(p).wait_send()


def backward_kernel(
    groups, pitch, early, table_high, table_low, partial, next_high, next_low,
    last_spectrum, last_left, last_right, last_moments, coefficients,
    solved, acc, last_high, last_low, left_states, right_states, stage, stored,
):
    _, steps, length = solved.shape
    rows = SEGMENTS * steps
    half = length // 2
    blocks = length // LANES
    tiles = half // TILE
    last = tiles - 1

    def multiply(t, high, low, base, n):
        columns = tile_columns(n)
        inner = slice(t * TILE, (t + 1) * TILE)
        values = []
        for h in range(2):
            place = slice(h * rows, (h + 1) * rows)
            values.append(
                base[place, columns]
                + product(high[place, :], low[place, :], table_high[inner, columns], table_low[inner, columns])
            )
        return values

    for n in range(early, tiles):
        acc[:rows, tile_columns(n)], acc[rows:, tile_columns(n)] = multiply(last - 1, next_high, next_low, partial, n)
    row_values = [coefficients[i, last:tiles, :] for i in range(COEFFICIENTS)]
    boundary_states(
        groups, lambda index: last_moments[index], row_values,
        last_left, last_right, left_states, right_states, slice(0, 2 * TILE),
    )
    solve_lines(last_spectrum, row_values[0], left_states, right_states, last_high, last_low)
    signs = parity((SEGMENTS, LANES))
    copies = []
    ready = []
    for n in range(tiles):
        while len(ready) < min(n + AHEAD, tiles):
            m = len(ready)
            ready.append(multiply(last, last_high, last_low, partial if m < early else acc, m))
        odds, evens = ready[n]
        for c in range(TILE // LANES):
            near = n * TILE // LANES + c
            far = blocks - 1 - near
            lanes = slice(c * LANES, (c + 1) * LANES)
            for g in range(steps):
                place = pl.ds(g, SEGMENTS, stride=pitch)
                odd = odds[g * SEGMENTS : (g + 1) * SEGMENTS, lanes]
                even = evens[g * SEGMENTS : (g + 1) * SEGMENTS, lanes] * signs
                stage[near, place, :] = even + odd
                stage[far, place, :] = mirrored(even - odd)
        for c in range(TILE // LANES):
            near = n * TILE // LANES + c
            for index in (near, blocks - 1 - near):
                copy = pltpu.make_async_copy(
                    stage.at[index].reshape(SEGMENTS, pitch, LANES).at[:, pl.ds(0, steps), :],
                    solved.at[:, :, pl.ds(index * LANES, LANES)],
                    stored.at[index],
                )
                copy.start()
                copies.append(copy)
    for copy in copies:
        copy.wait()


def on_device(source, screening):
    groups = lax.axis_size(GRID_AXES)
    fields, rows, length = source.shape
    half = length // 2
    tiles = half // TILE
    width = 2 * TILE
    steps = rows // SEGMENTS
    pitch = steps + 8 if steps % 16 == 0 else steps
    blocks = length // LANES
    constants = jnp.asarray(constant_rows(length))
    cosines = jnp.asarray(cosine_rows(length))
    vmem = pl.BlockSpec(memory_space=pltpu.VMEM)
    hbm = pl.BlockSpec(memory_space=pl.ANY)
    f32 = lambda *shape: jax.ShapeDtypeStruct(shape, jnp.float32)
    bf16 = lambda *shape: jax.ShapeDtypeStruct(shape, jnp.bfloat16)
    stay = lambda array: pltpu.with_memory_space_constraint(array, pltpu.HBM)
    floats = lambda *shape: pltpu.VMEM(shape, jnp.float32)
    halves = lambda *shape: pltpu.VMEM(shape, jnp.bfloat16)
    staging = [floats(blocks, SEGMENTS * pitch, LANES), pltpu.SemaphoreType.DMA((blocks,))]

    def one_field(grid, constant):
        parts = pl.pallas_call(
            functools.partial(forward_kernel, groups, pitch, tiles // 2),
            out_shape=[
                bf16(half, half), bf16(half, half), f32(2 * rows, half),
                bf16(2 * rows, TILE), bf16(2 * rows, TILE),
                f32(rows, width), f32(SEGMENTS, width), f32(SEGMENTS, width),
                f32(groups, 2, width), f32(COEFFICIENTS, *cosines.shape),
            ],
            in_specs=[hbm, pl.BlockSpec(memory_space=pltpu.SMEM), hbm, hbm],
            out_specs=[vmem] * 10,
            scratch_shapes=[
                floats(*constants.shape), pltpu.SemaphoreType.DMA((tiles,)),
                floats(*cosines.shape), pltpu.SemaphoreType.DMA((1,)),
            ]
            + staging
            + [halves(2 * rows, half)] * 2
            + [halves(tiles - 1, 2 * rows, TILE)] * 2
            + [floats(tiles - 1, rows, width)]
            + [floats(tiles - 1, SEGMENTS, width)] * 4
            + [floats(tiles, groups, 2, width)]
            + [pltpu.SemaphoreType.DMA((tiles + 1,))] * 2,
            compiler_params=pltpu.CompilerParams(
                vmem_limit_bytes=40 * 2**20, collective_id=0, has_side_effects=True
            ),
            name="forward",
        )(stay(grid.reshape(SEGMENTS, steps, length)), constant, stay(constants), stay(cosines))
        solved = pl.pallas_call(
            functools.partial(backward_kernel, groups, pitch, tiles // 2),
            out_shape=f32(SEGMENTS, steps, length),
            in_specs=[vmem] * 10,
            out_specs=hbm,
            scratch_shapes=[floats(2 * rows, half)]
            + [halves(2 * rows, TILE)] * 2
            + [floats(SEGMENTS, width)] * 2
            + staging,
            compiler_params=pltpu.CompilerParams(vmem_limit_bytes=40 * 2**20),
            name="backward",
        )(*parts)
        return solved.reshape(rows, length)

    return jnp.stack([one_field(source[f], screening[f : f + 1]) for f in range(fields)])


def solution(mesh):
    return jax.shard_map(
        on_device,
        mesh=mesh,
        in_specs=(P("af", GRID_AXES, None), P("af")),
        out_specs=P("af", GRID_AXES, None),
        check_vma=False,
    )
```

```python
import functools
import math

import jax
import jax.numpy as jnp
import numpy as np
from jax import lax
from jax.experimental import pallas as pl
from jax.experimental.pallas import tpu as pltpu
from jax.sharding import PartitionSpec as P

LANES = 128
SEGMENTS = 8
TILE = 256
STEP = 32
COEFFICIENTS = 6
AHEAD = 2
GRID_AXES = ("gx", "gy")
MESH = pl.DeviceIdType.MESH


def mode_numbers(length):
    half = length // 2
    numbers = np.arange(half, dtype=np.int64) + 1
    return np.concatenate([2 * numbers, length + 1 - 2 * numbers])


def double_cosines(length):
    angles = mode_numbers(length).astype(np.float32) * np.float32(math.pi / (length + 1))
    return np.float32(2.0) * np.cos(angles.astype(np.float64)).astype(np.float32)


def constant_rows(length):
    half = length // 2
    columns = np.arange(half, dtype=np.int64)[None, :] + 1
    coarse = np.arange(half // STEP, dtype=np.int64)[:, None] * STEP
    fine = np.arange(STEP, dtype=np.int64)[:, None] + 1
    scale = math.sqrt(2.0 / (length + 1))
    angle = lambda rows: 2.0 * math.pi * (rows * columns % (length + 1)) / (length + 1)
    tables = (
        scale * np.sin(angle(coarse)),
        scale * np.cos(angle(coarse)),
        np.sin(angle(fine)),
        np.cos(angle(fine)),
    )
    return np.concatenate(tables).astype(np.float32)


def cosine_rows(length):
    tiles = length // (2 * TILE)
    rows = double_cosines(length).reshape(2, tiles, TILE).transpose(1, 0, 2).reshape(tiles, 2 * TILE)
    return np.concatenate([rows, np.repeat(rows[-1:], -tiles % SEGMENTS, axis=0)])


def power(base, exponent):
    result = None
    while exponent:
        if exponent & 1:
            result = base if result is None else result * base
        exponent >>= 1
        if exponent:
            base = base * base
    return result


def decay_of(screening, cosines):
    factor = (4.0 + screening) - cosines
    excess = factor - 2.0
    root = jnp.sqrt(excess * (excess + 4.0))
    return 2.0 / (factor + root), root


def split(values):
    high = values.astype(jnp.bfloat16)
    return high, (values - high.astype(jnp.float32)).astype(jnp.bfloat16)


def mirrored(values):
    lanes = lax.broadcasted_iota(jnp.int32, values.shape, 1)
    return jnp.take_along_axis(values, LANES - 1 - lanes, axis=1)


def parity(shape):
    lanes = lax.broadcasted_iota(jnp.int32, shape, 1)
    return jnp.where(lanes % 2 == 0, 1.0, -1.0)


def tile_columns(t):
    return slice(t * TILE, (t + 1) * TILE)


def product(high, low, table_high, table_low):
    dot = functools.partial(jnp.dot, preferred_element_type=jnp.float32)
    return dot(high, table_high) + dot(low, table_high) + dot(high, table_low)


def peer(index):
    across = lax.axis_size("gy")
    return {"gx": index // across, "gy": index % across}


def store_coefficients(groups, rows, screening, cosines, coefficients):
    decay, root = decay_of(screening, cosines)
    whole = power(decay, rows * groups + 1)
    values = (
        decay,
        power(decay, rows // SEGMENTS),
        power(decay, rows),
        whole,
        -decay / (1.0 - whole * whole),
        1.0 / root,
    )
    for index, value in enumerate(values):
        coefficients[index] = value


def boundary_states(groups, moments_of, coefficients, left_parts, right_parts, left_states, right_states, columns):
    decay, stride, block, whole, edge, scale = coefficients
    position = lax.axis_index(GRID_AXES)
    moments = [moments_of((position + groups - d) % groups) for d in range(groups)]
    left_total = right_total = jnp.zeros_like(decay)
    for d in range(groups):
        left_total = block * left_total + moments[d][0:1, :]
        right_total = block * right_total + moments[groups - 1 - d][1:2, :]
    left_state = edge * (right_total - whole * left_total)
    right_state = edge * (left_total - whole * right_total)
    left_own, right_own = left_state, right_state
    for d in range(groups):
        left_own = jnp.where(d == position, left_state, left_own)
        left_state = block * left_state + moments[d][0:1, :]
        e = groups - 1 - d
        right_own = jnp.where(e == position, right_state, right_own)
        right_state = block * right_state + moments[e][1:2, :]
    after_states = []
    for s in range(SEGMENTS):
        left_states[s : s + 1, columns] = left_own
        left_own = stride * left_own + left_parts[s : s + 1, columns]
        after_states.append(left_own)
    for s in reversed(range(SEGMENTS)):
        right_states[s : s + 1, columns] = (right_own + decay * after_states[s]) * scale
        right_own = stride * right_own + right_parts[s : s + 1, columns]


def solve_lines(spectrum, decay, left_states, right_states, high, low, parts=(0, 1)):
    rows = spectrum.shape[0]
    steps = rows // SEGMENTS
    for h in parts:
        columns = tile_columns(h)
        ratio = jnp.broadcast_to(decay[:, columns], (SEGMENTS, TILE))
        state = left_states[:, columns]
        sums = []
        for g in range(steps):
            state = ratio * state + spectrum[g * SEGMENTS : (g + 1) * SEGMENTS, columns]
            sums.append(state)
        state = right_states[:, columns]
        for g in reversed(range(0, steps, 2)):
            later = ratio * (state + sums[g + 1])
            state = ratio * (later + sums[g])
            place = pl.ds((h - parts[0]) * rows + g * SEGMENTS, 2 * SEGMENTS)
            high[place, :], low[place, :] = split(jnp.concatenate([state, later], axis=0))


def line_sums(spectrum, decay, stride, left_parts, right_parts, moments, parts=(0, 1)):
    rows = spectrum.shape[0]
    steps = rows // SEGMENTS
    for h in parts:
        columns = tile_columns(h)
        ratio = jnp.broadcast_to(decay[:, columns], (SEGMENTS, TILE))
        left = right = jnp.zeros((SEGMENTS, TILE), jnp.float32)
        for g in range(steps):
            mirror = steps - 1 - g
            left = ratio * left + spectrum[g * SEGMENTS : (g + 1) * SEGMENTS, columns]
            right = ratio * right + spectrum[mirror * SEGMENTS : (mirror + 1) * SEGMENTS, columns]
        left_parts[:, columns] = left
        right_parts[:, columns] = right
        jump = stride[:, columns]
        left = right = jnp.zeros_like(jump)
        for s in range(SEGMENTS):
            left = jump * left + left_parts[s : s + 1, columns]
            right = jump * right + right_parts[SEGMENTS - 1 - s : SEGMENTS - s, columns]
        moments[0:1, columns] = left
        moments[1:2, columns] = right


def forward_kernel(
    groups, pitch, early, source, screening, constants, cosines,
    table_high, table_low, partial, next_high, next_low,
    last_spectrum, last_left, last_right, last_moments, coefficients,
    angles, angle_sems, cosines_here, cosines_sem, stage, arrived, high, low, back_high, back_low,
    spectrum, left_parts, right_parts, left_states, right_states,
    landed, send_sems, recv_sems,
):
    _, steps, length = source.shape
    rows = SEGMENTS * steps
    half = length // 2
    blocks = length // LANES
    tiles = half // TILE
    last = tiles - 1
    position = lax.axis_index(GRID_AXES)

    angle_copies = [
        pltpu.make_async_copy(
            constants.at[:, pl.ds(t * TILE, TILE)], angles.at[:, pl.ds(t * TILE, TILE)], angle_sems.at[t]
        )
        for t in range(tiles)
    ]
    cosines_copy = pltpu.make_async_copy(cosines, cosines_here, cosines_sem.at[0])
    copies = [
        pltpu.make_async_copy(
            source.at[:, :, pl.ds(c * LANES, LANES)],
            stage.at[c].reshape(SEGMENTS, pitch, LANES).at[:, pl.ds(0, steps), :],
            arrived.at[c],
        )
        for c in range(blocks)
    ]
    angle_copies[0].start()
    cosines_copy.start()
    for c in range(blocks // 2):
        copies[c].start()
        copies[blocks - 1 - c].start()
    for copy in angle_copies[1:]:
        copy.start()
    barrier = pltpu.get_barrier_semaphore()
    for d in range(1, groups):
        pl.semaphore_signal(barrier, inc=1, device_id=peer((position + d) % groups), device_id_type=MESH)

    coarse_rows = half // STEP

    def make_table(t):
        columns = tile_columns(t)
        fine_sin = angles[2 * coarse_rows : 2 * coarse_rows + STEP, columns]
        fine_cos = angles[2 * coarse_rows + STEP : 2 * coarse_rows + 2 * STEP, columns]
        for a in range(coarse_rows):
            coarse_sin = angles[a : a + 1, columns]
            coarse_cos = angles[coarse_rows + a : coarse_rows + a + 1, columns]
            place = slice(a * STEP, (a + 1) * STEP)
            table_high[place, columns], table_low[place, columns] = split(coarse_sin * fine_cos + coarse_cos * fine_sin)

    def row_of(index, t):
        return coefficients[index, t : t + 1, :]

    angle_copies[0].wait()
    cosines_copy.wait()
    store_coefficients(groups, rows, screening[0], cosines_here[...], coefficients)
    make_table(0)
    signs = parity((2 * SEGMENTS, LANES))
    pairs = blocks // 2
    for begin in range(0, pairs, pairs // 2):
        chosen = range(begin, begin + pairs // 2)
        for c in chosen:
            copies[c].wait()
            copies[blocks - 1 - c].wait()
        if begin:
            for copy in angle_copies[1:]:
                copy.wait()
            pl.semaphore_wait(barrier, groups - 1)
        for c in chosen:
            columns = pl.ds(c * LANES, LANES)
            for g in range(0, steps, 2):
                place = pl.ds(g * SEGMENTS, 2 * SEGMENTS)
                place_sum = pl.ds(rows + g * SEGMENTS, 2 * SEGMENTS)

                def load(column):
                    pair = [stage[column, pl.ds(g + e, SEGMENTS, stride=pitch), :] for e in range(2)]
                    return jnp.concatenate(pair, axis=0)

                near = load(c)
                far = mirrored(load(blocks - 1 - c))
                high[place, columns], low[place, columns] = split(near - far)
                high[place_sum, columns], low[place_sum, columns] = split((near + far) * signs)
    def lines_of(t):
        return last_spectrum if t == last else spectrum.at[t]

    def sums_of(t):
        return (last_left, last_right) if t == last else (left_parts.at[t], right_parts.at[t])

    def transform(t, h, begin=0, end=2):
        columns = tile_columns(t)
        inner = slice(begin * half // 2, end * half // 2)
        for k in range(2):
            part = slice(k * rows // 2, (k + 1) * rows // 2)
            place = slice(h * rows + k * rows // 2, h * rows + (k + 1) * rows // 2)
            values = product(
                high[place, inner], low[place, inner], table_high[inner, columns], table_low[inner, columns]
            )
            target = lines_of(t)
            target[part, tile_columns(h)] = target[part, tile_columns(h)] + values if begin else values

    every = (0, 1)
    whole_tile = slice(0, 2 * TILE)
    parcels = [(t, every, whole_tile) for t in range(last)] + [(last, (h,), tile_columns(h)) for h in every]

    def sum_lines(t, parts=every):
        line_sums(lines_of(t), row_of(0, t), row_of(1, t), *sums_of(t), landed.at[t, 0], parts)

    def send(p):
        t, _, columns = parcels[p]
        for d in range(1, groups):
            pltpu.make_async_remote_copy(
                src_ref=landed.at[t, 0, :, columns],
                dst_ref=landed.at[t, d, :, columns],
                send_sem=send_sems.at[p],
                recv_sem=recv_sems.at[p],
                device_id=peer((position + d) % groups),
                device_id_type=MESH,
            ).start()

    def all_of(p):
        t, _, columns = parcels[p]
        ref = landed.at[t, pl.ds(1, groups - 1), :, columns]
        return pltpu.make_async_remote_copy(
            src_ref=ref,
            dst_ref=ref,
            send_sem=send_sems.at[p],
            recv_sem=recv_sems.at[p],
            device_id=peer((position + 1) % groups),
            device_id_type=MESH,
        )

    for t in range(tiles):
        if t:
            transform(t, 0, 0, 1)
            sum_lines(t - 1, (1,))
            send(t - 1)
            transform(t, 0, 1, 2)
        else:
            transform(t, 0)
        transform(t, 1)
        if t < last:
            make_table(t + 1)
        sum_lines(t, (0,))
    send(last)
    sum_lines(last, (1,))
    send(tiles)

    def multiply(t, high, low, chosen):
        inner = slice(t * TILE, (t + 1) * TILE)
        for n in chosen:
            columns = tile_columns(n)
            for h in every:
                place = slice(h * rows, (h + 1) * rows)
                values = product(high[place, :], low[place, :], table_high[inner, columns], table_low[inner, columns])
                partial[place, columns] = values if t == 0 else partial[place, columns] + values

    def target_of(t):
        return (next_high, next_low) if t == last - 1 else (back_high.at[t], back_low.at[t])

    for t in range(last):
        all_of(t).wait_recv()
        if t:
            multiply(t - 1, *target_of(t - 1), (tiles - 1,))
        boundary_states(
            groups, lambda index: landed[t, index], [row_of(i, t) for i in range(COEFFICIENTS)],
            *sums_of(t), left_states.at[t], right_states.at[t], whole_tile,
        )
        solve_lines(lines_of(t), row_of(0, t), left_states.at[t], right_states.at[t], *target_of(t))
        multiply(t, *target_of(t), range(early if t == last - 1 else tiles - 1))
    all_of(last).wait_recv()
    all_of(tiles).wait_recv()
    for d in range(groups):
        last_moments[d] = landed[last, d]
    for p in range(tiles + 1):
        all_of(p).wait_send()


def backward_kernel(
    groups, pitch, early, table_high, table_low, partial, next_high, next_low,
    last_spectrum, last_left, last_right, last_moments, coefficients,
    solved, acc, last_high, last_low, left_states, right_states, stage, stored,
):
    _, steps, length = solved.shape
    rows = SEGMENTS * steps
    half = length // 2
    blocks = length // LANES
    tiles = half // TILE
    last = tiles - 1

    def multiply(t, high, low, base, n):
        columns = tile_columns(n)
        inner = slice(t * TILE, (t + 1) * TILE)
        values = []
        for h in range(2):
            place = slice(h * rows, (h + 1) * rows)
            values.append(
                base[place, columns]
                + product(high[place, :], low[place, :], table_high[inner, columns], table_low[inner, columns])
            )
        return values

    for n in range(early, tiles):
        acc[:rows, tile_columns(n)], acc[rows:, tile_columns(n)] = multiply(last - 1, next_high, next_low, partial, n)
    row_values = [coefficients[i, last:tiles, :] for i in range(COEFFICIENTS)]
    boundary_states(
        groups, lambda index: last_moments[index], row_values,
        last_left, last_right, left_states, right_states, slice(0, 2 * TILE),
    )
    solve_lines(last_spectrum, row_values[0], left_states, right_states, last_high, last_low)
    signs = parity((SEGMENTS, LANES))
    copies = []
    ready = []
    for n in range(tiles):
        while len(ready) < min(n + AHEAD, tiles):
            m = len(ready)
            ready.append(multiply(last, last_high, last_low, partial if m < early else acc, m))
        odds, evens = ready[n]
        for c in range(TILE // LANES):
            near = n * TILE // LANES + c
            far = blocks - 1 - near
            lanes = slice(c * LANES, (c + 1) * LANES)
            for g in range(steps):
                place = pl.ds(g, SEGMENTS, stride=pitch)
                odd = odds[g * SEGMENTS : (g + 1) * SEGMENTS, lanes]
                even = evens[g * SEGMENTS : (g + 1) * SEGMENTS, lanes] * signs
                stage[near, place, :] = even + odd
                stage[far, place, :] = mirrored(even - odd)
        for c in range(TILE // LANES):
            near = n * TILE // LANES + c
            for index in (near, blocks - 1 - near):
                copy = pltpu.make_async_copy(
                    stage.at[index].reshape(SEGMENTS, pitch, LANES).at[:, pl.ds(0, steps), :],
                    solved.at[:, :, pl.ds(index * LANES, LANES)],
                    stored.at[index],
                )
                copy.start()
                copies.append(copy)
    for copy in copies:
        copy.wait()


def on_device(source, screening):
    groups = lax.axis_size(GRID_AXES)
    fields, rows, length = source.shape
    half = length // 2
    tiles = half // TILE
    width = 2 * TILE
    steps = rows // SEGMENTS
    pitch = steps + 8 if steps % 16 == 0 else steps
    blocks = length // LANES
    constants = jnp.asarray(constant_rows(length))
    cosines = jnp.asarray(cosine_rows(length))
    vmem = pl.BlockSpec(memory_space=pltpu.VMEM)
    hbm = pl.BlockSpec(memory_space=pl.ANY)
    f32 = lambda *shape: jax.ShapeDtypeStruct(shape, jnp.float32)
    bf16 = lambda *shape: jax.ShapeDtypeStruct(shape, jnp.bfloat16)
    stay = lambda array: pltpu.with_memory_space_constraint(array, pltpu.HBM)
    floats = lambda *shape: pltpu.VMEM(shape, jnp.float32)
    halves = lambda *shape: pltpu.VMEM(shape, jnp.bfloat16)
    staging = [floats(blocks, SEGMENTS * pitch, LANES), pltpu.SemaphoreType.DMA((blocks,))]

    def one_field(grid, constant):
        parts = pl.pallas_call(
            functools.partial(forward_kernel, groups, pitch, tiles // 2),
            out_shape=[
                bf16(half, half), bf16(half, half), f32(2 * rows, half),
                bf16(2 * rows, TILE), bf16(2 * rows, TILE),
                f32(rows, width), f32(SEGMENTS, width), f32(SEGMENTS, width),
                f32(groups, 2, width), f32(COEFFICIENTS, *cosines.shape),
            ],
            in_specs=[hbm, pl.BlockSpec(memory_space=pltpu.SMEM), hbm, hbm],
            out_specs=[vmem] * 10,
            scratch_shapes=[
                floats(*constants.shape), pltpu.SemaphoreType.DMA((tiles,)),
                floats(*cosines.shape), pltpu.SemaphoreType.DMA((1,)),
            ]
            + staging
            + [halves(2 * rows, half)] * 2
            + [halves(tiles - 1, 2 * rows, TILE)] * 2
            + [floats(tiles - 1, rows, width)]
            + [floats(tiles - 1, SEGMENTS, width)] * 4
            + [floats(tiles, groups, 2, width)]
            + [pltpu.SemaphoreType.DMA((tiles + 1,))] * 2,
            compiler_params=pltpu.CompilerParams(
                vmem_limit_bytes=40 * 2**20, collective_id=0, has_side_effects=True
            ),
            name="forward",
        )(stay(grid.reshape(SEGMENTS, steps, length)), constant, stay(constants), stay(cosines))
        solved = pl.pallas_call(
            functools.partial(backward_kernel, groups, pitch, tiles // 2),
            out_shape=f32(SEGMENTS, steps, length),
            in_specs=[vmem] * 10,
            out_specs=hbm,
            scratch_shapes=[floats(2 * rows, half)]
            + [halves(2 * rows, TILE)] * 2
            + [floats(SEGMENTS, width)] * 2
            + staging,
            compiler_params=pltpu.CompilerParams(vmem_limit_bytes=40 * 2**20),
            name="backward",
        )(*parts)
        return solved.reshape(rows, length)

    return jnp.stack([one_field(source[f], screening[f : f + 1]) for f in range(fields)])


def solution(mesh):
    return jax.shard_map(
        on_device,
        mesh=mesh,
        in_specs=(P("af", GRID_AXES, None), P("af")),
        out_specs=P("af", GRID_AXES, None),
        check_vma=False,
    )
```

```python
import functools
import math

import jax
import jax.numpy as jnp
import numpy as np
from jax import lax
from jax.experimental import pallas as pl
from jax.experimental.pallas import tpu as pltpu
from jax.sharding import PartitionSpec as P

LANES = 128
SEGMENTS = 8
TILE = 256
STEP = 32
COEFFICIENTS = 6
AHEAD = 2
GRID_AXES = ("gx", "gy")
MESH = pl.DeviceIdType.MESH


def mode_numbers(length):
    half = length // 2
    numbers = np.arange(half, dtype=np.int64) + 1
    return np.concatenate([2 * numbers, length + 1 - 2 * numbers])


def double_cosines(length):
    angles = mode_numbers(length).astype(np.float32) * np.float32(math.pi / (length + 1))
    return np.float32(2.0) * np.cos(angles.astype(np.float64)).astype(np.float32)


def constant_rows(length):
    half = length // 2
    columns = np.arange(half, dtype=np.int64)[None, :] + 1
    coarse = np.arange(half // STEP, dtype=np.int64)[:, None] * STEP
    fine = np.arange(STEP, dtype=np.int64)[:, None] + 1
    scale = math.sqrt(2.0 / (length + 1))
    angle = lambda rows: 2.0 * math.pi * (rows * columns % (length + 1)) / (length + 1)
    tables = (
        scale * np.sin(angle(coarse)),
        scale * np.cos(angle(coarse)),
        np.sin(angle(fine)),
        np.cos(angle(fine)),
    )
    return np.concatenate(tables).astype(np.float32)


def cosine_rows(length):
    tiles = length // (2 * TILE)
    rows = double_cosines(length).reshape(2, tiles, TILE).transpose(1, 0, 2).reshape(tiles, 2 * TILE)
    return np.concatenate([rows, np.repeat(rows[-1:], -tiles % SEGMENTS, axis=0)])


def power(base, exponent):
    result = None
    while exponent:
        if exponent & 1:
            result = base if result is None else result * base
        exponent >>= 1
        if exponent:
            base = base * base
    return result


def decay_of(screening, cosines):
    factor = (4.0 + screening) - cosines
    excess = factor - 2.0
    root = jnp.sqrt(excess * (excess + 4.0))
    return 2.0 / (factor + root), root


def split(values):
    high = values.astype(jnp.bfloat16)
    return high, (values - high.astype(jnp.float32)).astype(jnp.bfloat16)


def mirrored(values):
    lanes = lax.broadcasted_iota(jnp.int32, values.shape, 1)
    return jnp.take_along_axis(values, LANES - 1 - lanes, axis=1)


def parity(shape):
    lanes = lax.broadcasted_iota(jnp.int32, shape, 1)
    return jnp.where(lanes % 2 == 0, 1.0, -1.0)


def tile_columns(t):
    return slice(t * TILE, (t + 1) * TILE)


def product(high, low, table_high, table_low):
    dot = functools.partial(jnp.dot, preferred_element_type=jnp.float32)
    return dot(high, table_high) + dot(low, table_high) + dot(high, table_low)


def peer(index):
    across = lax.axis_size("gy")
    return {"gx": index // across, "gy": index % across}


def store_coefficients(groups, rows, screening, cosines, coefficients):
    decay, root = decay_of(screening, cosines)
    whole = power(decay, rows * groups + 1)
    values = (
        decay,
        power(decay, rows // SEGMENTS),
        power(decay, rows),
        whole,
        -decay / (1.0 - whole * whole),
        1.0 / root,
    )
    for index, value in enumerate(values):
        coefficients[index] = value


def boundary_states(groups, moments_of, coefficients, left_parts, right_parts, left_states, right_states, columns):
    decay, stride, block, whole, edge, scale = coefficients
    position = lax.axis_index(GRID_AXES)
    moments = [moments_of((position + groups - d) % groups) for d in range(groups)]
    left_total = right_total = jnp.zeros_like(decay)
    for d in range(groups):
        left_total = block * left_total + moments[d][0:1, :]
        right_total = block * right_total + moments[groups - 1 - d][1:2, :]
    left_state = edge * (right_total - whole * left_total)
    right_state = edge * (left_total - whole * right_total)
    left_own, right_own = left_state, right_state
    for d in range(groups):
        left_own = jnp.where(d == position, left_state, left_own)
        left_state = block * left_state + moments[d][0:1, :]
        e = groups - 1 - d
        right_own = jnp.where(e == position, right_state, right_own)
        right_state = block * right_state + moments[e][1:2, :]
    after_states = []
    for s in range(SEGMENTS):
        left_states[s : s + 1, columns] = left_own
        left_own = stride * left_own + left_parts[s : s + 1, columns]
        after_states.append(left_own)
    for s in reversed(range(SEGMENTS)):
        right_states[s : s + 1, columns] = (right_own + decay * after_states[s]) * scale
        right_own = stride * right_own + right_parts[s : s + 1, columns]


def solve_lines(spectrum, decay, left_states, right_states, high, low, parts=(0, 1)):
    rows = spectrum.shape[0]
    steps = rows // SEGMENTS
    for h in parts:
        columns = tile_columns(h)
        ratio = jnp.broadcast_to(decay[:, columns], (SEGMENTS, TILE))
        state = left_states[:, columns]
        sums = []
        for g in range(steps):
            state = ratio * state + spectrum[g * SEGMENTS : (g + 1) * SEGMENTS, columns]
            sums.append(state)
        state = right_states[:, columns]
        for g in reversed(range(0, steps, 2)):
            later = ratio * (state + sums[g + 1])
            state = ratio * (later + sums[g])
            place = pl.ds((h - parts[0]) * rows + g * SEGMENTS, 2 * SEGMENTS)
            high[place, :], low[place, :] = split(jnp.concatenate([state, later], axis=0))


def line_sums(spectrum, decay, stride, left_parts, right_parts, moments, parts=(0, 1)):
    rows = spectrum.shape[0]
    steps = rows // SEGMENTS
    for h in parts:
        columns = tile_columns(h)
        ratio = jnp.broadcast_to(decay[:, columns], (SEGMENTS, TILE))
        left = right = jnp.zeros((SEGMENTS, TILE), jnp.float32)
        for g in range(steps):
            mirror = steps - 1 - g
            left = ratio * left + spectrum[g * SEGMENTS : (g + 1) * SEGMENTS, columns]
            right = ratio * right + spectrum[mirror * SEGMENTS : (mirror + 1) * SEGMENTS, columns]
        left_parts[:, columns] = left
        right_parts[:, columns] = right
        jump = stride[:, columns]
        left = right = jnp.zeros_like(jump)
        for s in range(SEGMENTS):
            left = jump * left + left_parts[s : s + 1, columns]
            right = jump * right + right_parts[SEGMENTS - 1 - s : SEGMENTS - s, columns]
        moments[0:1, columns] = left
        moments[1:2, columns] = right


def forward_kernel(
    groups, pitch, early, source, screening, constants, cosines,
    table_high, table_low, partial, next_high, next_low,
    last_spectrum, last_left, last_right, last_moments, coefficients,
    angles, angle_sems, cosines_here, cosines_sem, stage, arrived, high, low, back_high, back_low,
    spectrum, left_parts, right_parts, left_states, right_states,
    landed, send_sems, recv_sems,
):
    _, steps, length = source.shape
    rows = SEGMENTS * steps
    half = length // 2
    blocks = length // LANES
    tiles = half // TILE
    last = tiles - 1
    position = lax.axis_index(GRID_AXES)

    angle_copies = [
        pltpu.make_async_copy(
            constants.at[:, pl.ds(t * TILE, TILE)], angles.at[:, pl.ds(t * TILE, TILE)], angle_sems.at[t]
        )
        for t in range(tiles)
    ]
    cosines_copy = pltpu.make_async_copy(cosines, cosines_here, cosines_sem.at[0])
    copies = [
        pltpu.make_async_copy(
            source.at[:, :, pl.ds(c * LANES, LANES)],
            stage.at[c].reshape(SEGMENTS, pitch, LANES).at[:, pl.ds(0, steps), :],
            arrived.at[c],
        )
        for c in range(blocks)
    ]
    angle_copies[0].start()
    cosines_copy.start()
    for c in range(blocks // 2):
        copies[c].start()
        copies[blocks - 1 - c].start()
    for copy in angle_copies[1:]:
        copy.start()
    barrier = pltpu.get_barrier_semaphore()
    for d in range(1, groups):
        pl.semaphore_signal(barrier, inc=1, device_id=peer((position + d) % groups), device_id_type=MESH)

    coarse_rows = half // STEP

    def make_table(t):
        columns = tile_columns(t)
        fine_sin = angles[2 * coarse_rows : 2 * coarse_rows + STEP, columns]
        fine_cos = angles[2 * coarse_rows + STEP : 2 * coarse_rows + 2 * STEP, columns]
        for a in range(coarse_rows):
            coarse_sin = angles[a : a + 1, columns]
            coarse_cos = angles[coarse_rows + a : coarse_rows + a + 1, columns]
            place = slice(a * STEP, (a + 1) * STEP)
            table_high[place, columns], table_low[place, columns] = split(coarse_sin * fine_cos + coarse_cos * fine_sin)

    def row_of(index, t):
        return coefficients[index, t : t + 1, :]

    angle_copies[0].wait()
    cosines_copy.wait()
    store_coefficients(groups, rows, screening[0], cosines_here[...], coefficients)
    make_table(0)
    signs = parity((2 * SEGMENTS, LANES))
    pairs = blocks // 2
    for begin in range(0, pairs, pairs // 2):
        chosen = range(begin, begin + pairs // 2)
        for c in chosen:
            copies[c].wait()
            copies[blocks - 1 - c].wait()
        if begin:
            for copy in angle_copies[1:]:
                copy.wait()
            pl.semaphore_wait(barrier, groups - 1)
        for c in chosen:
            columns = pl.ds(c * LANES, LANES)
            for g in range(0, steps, 2):
                place = pl.ds(g * SEGMENTS, 2 * SEGMENTS)
                place_sum = pl.ds(rows + g * SEGMENTS, 2 * SEGMENTS)

                def load(column):
                    pair = [stage[column, pl.ds(g + e, SEGMENTS, stride=pitch), :] for e in range(2)]
                    return jnp.concatenate(pair, axis=0)

                near = load(c)
                far = mirrored(load(blocks - 1 - c))
                high[place, columns], low[place, columns] = split(near - far)
                high[place_sum, columns], low[place_sum, columns] = split((near + far) * signs)
    def lines_of(t):
        return last_spectrum if t == last else spectrum.at[t]

    def sums_of(t):
        return (last_left, last_right) if t == last else (left_parts.at[t], right_parts.at[t])

    def transform(t, h):
        columns = tile_columns(t)
        for k in range(2):
            part = slice(k * rows // 2, (k + 1) * rows // 2)
            place = slice(h * rows + k * rows // 2, h * rows + (k + 1) * rows // 2)
            lines_of(t)[part, tile_columns(h)] = product(
                high[place, :], low[place, :], table_high[:, columns], table_low[:, columns]
            )

    every = (0, 1)
    whole_tile = slice(0, 2 * TILE)

    def sum_lines(t):
        line_sums(lines_of(t), row_of(0, t), row_of(1, t), *sums_of(t), landed.at[t, 0])

    def send(t):
        for d in range(1, groups):
            pltpu.make_async_remote_copy(
                src_ref=landed.at[t, 0],
                dst_ref=landed.at[t, d],
                send_sem=send_sems.at[t],
                recv_sem=recv_sems.at[t],
                device_id=peer((position + d) % groups),
                device_id_type=MESH,
            ).start()

    def all_of(t):
        ref = landed.at[t, pl.ds(1, groups - 1)]
        return pltpu.make_async_remote_copy(
            src_ref=ref,
            dst_ref=ref,
            send_sem=send_sems.at[t],
            recv_sem=recv_sems.at[t],
            device_id=peer((position + 1) % groups),
            device_id_type=MESH,
        )

    for t in range(tiles):
        transform(t, 0)
        if t:
            sum_lines(t - 1)
            send(t - 1)
        transform(t, 1)
        if t < last:
            make_table(t + 1)
    sum_lines(last)
    send(last)

    def multiply(t, high, low, chosen):
        inner = slice(t * TILE, (t + 1) * TILE)
        for n in chosen:
            columns = tile_columns(n)
            for h in every:
                place = slice(h * rows, (h + 1) * rows)
                values = product(high[place, :], low[place, :], table_high[inner, columns], table_low[inner, columns])
                partial[place, columns] = values if t == 0 else partial[place, columns] + values

    def target_of(t):
        return (next_high, next_low) if t == last - 1 else (back_high.at[t], back_low.at[t])

    for t in range(last):
        all_of(t).wait_recv()
        if t:
            multiply(t - 1, *target_of(t - 1), (tiles - 1,))
        boundary_states(
            groups, lambda index: landed[t, index], [row_of(i, t) for i in range(COEFFICIENTS)],
            *sums_of(t), left_states.at[t], right_states.at[t], whole_tile,
        )
        solve_lines(lines_of(t), row_of(0, t), left_states.at[t], right_states.at[t], *target_of(t))
        multiply(t, *target_of(t), range(early if t == last - 1 else tiles - 1))
    all_of(last).wait_recv()
    for d in range(groups):
        last_moments[d] = landed[last, d]
    for t in range(tiles):
        all_of(t).wait_send()


def backward_kernel(
    groups, pitch, early, table_high, table_low, partial, next_high, next_low,
    last_spectrum, last_left, last_right, last_moments, coefficients,
    solved, acc, last_high, last_low, left_states, right_states, stage, stored,
):
    _, steps, length = solved.shape
    rows = SEGMENTS * steps
    half = length // 2
    blocks = length // LANES
    tiles = half // TILE
    last = tiles - 1

    def multiply(t, high, low, base, n):
        columns = tile_columns(n)
        inner = slice(t * TILE, (t + 1) * TILE)
        values = []
        for h in range(2):
            place = slice(h * rows, (h + 1) * rows)
            values.append(
                base[place, columns]
                + product(high[place, :], low[place, :], table_high[inner, columns], table_low[inner, columns])
            )
        return values

    for n in range(early, tiles):
        acc[:rows, tile_columns(n)], acc[rows:, tile_columns(n)] = multiply(last - 1, next_high, next_low, partial, n)
    row_values = [coefficients[i, last:tiles, :] for i in range(COEFFICIENTS)]
    boundary_states(
        groups, lambda index: last_moments[index], row_values,
        last_left, last_right, left_states, right_states, slice(0, 2 * TILE),
    )
    solve_lines(last_spectrum, row_values[0], left_states, right_states, last_high, last_low)
    signs = parity((SEGMENTS, LANES))
    copies = []
    ready = []

    def store(near):
        for index in (near, blocks - 1 - near):
            copy = pltpu.make_async_copy(
                stage.at[index].reshape(SEGMENTS, pitch, LANES).at[:, pl.ds(0, steps), :],
                solved.at[:, :, pl.ds(index * LANES, LANES)],
                stored.at[index],
            )
            copy.start()
            copies.append(copy)

    for n in range(tiles):
        while len(ready) < min(n + AHEAD, tiles):
            m = len(ready)
            ready.append(multiply(last, last_high, last_low, partial if m < early else acc, m))
        odds, evens = ready[n]
        for c in range(TILE // LANES):
            near = n * TILE // LANES + c
            far = blocks - 1 - near
            lanes = slice(c * LANES, (c + 1) * LANES)
            for g in range(steps):
                place = pl.ds(g, SEGMENTS, stride=pitch)
                odd = odds[g * SEGMENTS : (g + 1) * SEGMENTS, lanes]
                even = evens[g * SEGMENTS : (g + 1) * SEGMENTS, lanes] * signs
                stage[near, place, :] = even + odd
                stage[far, place, :] = mirrored(even - odd)
        for c in range(TILE // LANES):
            store(n * TILE // LANES + c)
    for copy in copies:
        copy.wait()


def on_device(source, screening):
    groups = lax.axis_size(GRID_AXES)
    fields, rows, length = source.shape
    half = length // 2
    tiles = half // TILE
    width = 2 * TILE
    steps = rows // SEGMENTS
    pitch = steps + 8 if steps % 16 == 0 else steps
    blocks = length // LANES
    constants = jnp.asarray(constant_rows(length))
    cosines = jnp.asarray(cosine_rows(length))
    vmem = pl.BlockSpec(memory_space=pltpu.VMEM)
    hbm = pl.BlockSpec(memory_space=pl.ANY)
    f32 = lambda *shape: jax.ShapeDtypeStruct(shape, jnp.float32)
    bf16 = lambda *shape: jax.ShapeDtypeStruct(shape, jnp.bfloat16)
    stay = lambda array: pltpu.with_memory_space_constraint(array, pltpu.HBM)
    floats = lambda *shape: pltpu.VMEM(shape, jnp.float32)
    halves = lambda *shape: pltpu.VMEM(shape, jnp.bfloat16)
    staging = [floats(blocks, SEGMENTS * pitch, LANES), pltpu.SemaphoreType.DMA((blocks,))]

    def one_field(grid, constant):
        parts = pl.pallas_call(
            functools.partial(forward_kernel, groups, pitch, tiles // 2),
            out_shape=[
                bf16(half, half), bf16(half, half), f32(2 * rows, half),
                bf16(2 * rows, TILE), bf16(2 * rows, TILE),
                f32(rows, width), f32(SEGMENTS, width), f32(SEGMENTS, width),
                f32(groups, 2, width), f32(COEFFICIENTS, *cosines.shape),
            ],
            in_specs=[hbm, pl.BlockSpec(memory_space=pltpu.SMEM), hbm, hbm],
            out_specs=[vmem] * 10,
            scratch_shapes=[
                floats(*constants.shape), pltpu.SemaphoreType.DMA((tiles,)),
                floats(*cosines.shape), pltpu.SemaphoreType.DMA((1,)),
            ]
            + staging
            + [halves(2 * rows, half)] * 2
            + [halves(tiles - 1, 2 * rows, TILE)] * 2
            + [floats(tiles - 1, rows, width)]
            + [floats(tiles - 1, SEGMENTS, width)] * 4
            + [floats(tiles, groups, 2, width)]
            + [pltpu.SemaphoreType.DMA((tiles,))] * 2,
            compiler_params=pltpu.CompilerParams(
                vmem_limit_bytes=40 * 2**20, collective_id=0, has_side_effects=True
            ),
            name="forward",
        )(stay(grid.reshape(SEGMENTS, steps, length)), constant, stay(constants), stay(cosines))
        solved = pl.pallas_call(
            functools.partial(backward_kernel, groups, pitch, tiles // 2),
            out_shape=f32(SEGMENTS, steps, length),
            in_specs=[vmem] * 10,
            out_specs=hbm,
            scratch_shapes=[floats(2 * rows, half)]
            + [halves(2 * rows, TILE)] * 2
            + [floats(SEGMENTS, width)] * 2
            + staging,
            compiler_params=pltpu.CompilerParams(vmem_limit_bytes=40 * 2**20),
            name="backward",
        )(*parts)
        return solved.reshape(rows, length)

    return jnp.stack([one_field(source[f], screening[f : f + 1]) for f in range(fields)])


def solution(mesh):
    return jax.shard_map(
        on_device,
        mesh=mesh,
        in_specs=(P("af", GRID_AXES, None), P("af")),
        out_specs=P("af", GRID_AXES, None),
        check_vma=False,
    )
```

```python
import functools
import math

import jax
import jax.numpy as jnp
import numpy as np
from jax import lax
from jax.experimental import pallas as pl
from jax.experimental.pallas import tpu as pltpu
from jax.sharding import PartitionSpec as P

LANES = 128
SEGMENTS = 8
TILE = 256
STEP = 32
COEFFICIENTS = 6
AHEAD = 2
FOLDS = 4
GRID_AXES = ("gx", "gy")
MESH = pl.DeviceIdType.MESH


def mode_numbers(length):
    half = length // 2
    numbers = np.arange(half, dtype=np.int64) + 1
    return np.concatenate([2 * numbers, length + 1 - 2 * numbers])


def double_cosines(length):
    angles = mode_numbers(length).astype(np.float32) * np.float32(math.pi / (length + 1))
    return np.float32(2.0) * np.cos(angles.astype(np.float64)).astype(np.float32)


def constant_rows(length):
    half = length // 2
    columns = np.arange(half, dtype=np.int64)[None, :] + 1
    coarse = np.arange(half // STEP, dtype=np.int64)[:, None] * STEP
    fine = np.arange(STEP, dtype=np.int64)[:, None] + 1
    scale = math.sqrt(2.0 / (length + 1))
    angle = lambda rows: 2.0 * math.pi * (rows * columns % (length + 1)) / (length + 1)
    tables = (
        scale * np.sin(angle(coarse)),
        scale * np.cos(angle(coarse)),
        np.sin(angle(fine)),
        np.cos(angle(fine)),
    )
    return np.concatenate(tables).astype(np.float32)


def cosine_rows(length):
    tiles = length // (2 * TILE)
    rows = double_cosines(length).reshape(2, tiles, TILE).transpose(1, 0, 2).reshape(tiles, 2 * TILE)
    return np.concatenate([rows, np.repeat(rows[-1:], -tiles % SEGMENTS, axis=0)])


def power(base, exponent):
    result = None
    while exponent:
        if exponent & 1:
            result = base if result is None else result * base
        exponent >>= 1
        if exponent:
            base = base * base
    return result


def decay_of(screening, cosines):
    factor = (4.0 + screening) - cosines
    excess = factor - 2.0
    root = jnp.sqrt(excess * (excess + 4.0))
    return 2.0 / (factor + root), root


def split(values):
    high = values.astype(jnp.bfloat16)
    return high, (values - high.astype(jnp.float32)).astype(jnp.bfloat16)


def mirrored(values):
    lanes = lax.broadcasted_iota(jnp.int32, values.shape, 1)
    return jnp.take_along_axis(values, LANES - 1 - lanes, axis=1)


def parity(shape):
    lanes = lax.broadcasted_iota(jnp.int32, shape, 1)
    return jnp.where(lanes % 2 == 0, 1.0, -1.0)


def tile_columns(t):
    return slice(t * TILE, (t + 1) * TILE)


def product(high, low, table_high, table_low):
    dot = functools.partial(jnp.dot, preferred_element_type=jnp.float32)
    return dot(high, table_high) + dot(low, table_high) + dot(high, table_low)


def peer(index):
    across = lax.axis_size("gy")
    return {"gx": index // across, "gy": index % across}


def store_coefficients(groups, rows, screening, cosines, coefficients):
    decay, root = decay_of(screening, cosines)
    whole = power(decay, rows * groups + 1)
    values = (
        decay,
        power(decay, rows // SEGMENTS),
        power(decay, rows),
        whole,
        -decay / (1.0 - whole * whole),
        1.0 / root,
    )
    for index, value in enumerate(values):
        coefficients[index] = value


def boundary_states(groups, moments_of, coefficients, left_parts, right_parts, left_states, right_states, columns):
    decay, stride, block, whole, edge, scale = coefficients
    position = lax.axis_index(GRID_AXES)
    moments = [moments_of((position + groups - d) % groups) for d in range(groups)]
    left_total = right_total = jnp.zeros_like(decay)
    for d in range(groups):
        left_total = block * left_total + moments[d][0:1, :]
        right_total = block * right_total + moments[groups - 1 - d][1:2, :]
    left_state = edge * (right_total - whole * left_total)
    right_state = edge * (left_total - whole * right_total)
    left_own, right_own = left_state, right_state
    for d in range(groups):
        left_own = jnp.where(d == position, left_state, left_own)
        left_state = block * left_state + moments[d][0:1, :]
        e = groups - 1 - d
        right_own = jnp.where(e == position, right_state, right_own)
        right_state = block * right_state + moments[e][1:2, :]
    after_states = []
    for s in range(SEGMENTS):
        left_states[s : s + 1, columns] = left_own
        left_own = stride * left_own + left_parts[s : s + 1, columns]
        after_states.append(left_own)
    for s in reversed(range(SEGMENTS)):
        right_states[s : s + 1, columns] = (right_own + decay * after_states[s]) * scale
        right_own = stride * right_own + right_parts[s : s + 1, columns]


def solve_lines(spectrum, decay, left_states, right_states, high, low, parts=(0, 1)):
    rows = spectrum.shape[0]
    steps = rows // SEGMENTS
    for h in parts:
        columns = tile_columns(h)
        ratio = jnp.broadcast_to(decay[:, columns], (SEGMENTS, TILE))
        state = left_states[:, columns]
        sums = []
        for g in range(steps):
            state = ratio * state + spectrum[g * SEGMENTS : (g + 1) * SEGMENTS, columns]
            sums.append(state)
        state = right_states[:, columns]
        for g in reversed(range(0, steps, 2)):
            later = ratio * (state + sums[g + 1])
            state = ratio * (later + sums[g])
            place = pl.ds((h - parts[0]) * rows + g * SEGMENTS, 2 * SEGMENTS)
            high[place, :], low[place, :] = split(jnp.concatenate([state, later], axis=0))


def line_sums(spectrum, decay, stride, left_parts, right_parts, moments, parts=(0, 1)):
    rows = spectrum.shape[0]
    steps = rows // SEGMENTS
    for h in parts:
        columns = tile_columns(h)
        ratio = jnp.broadcast_to(decay[:, columns], (SEGMENTS, TILE))
        left = right = jnp.zeros((SEGMENTS, TILE), jnp.float32)
        for g in range(steps):
            mirror = steps - 1 - g
            left = ratio * left + spectrum[g * SEGMENTS : (g + 1) * SEGMENTS, columns]
            right = ratio * right + spectrum[mirror * SEGMENTS : (mirror + 1) * SEGMENTS, columns]
        left_parts[:, columns] = left
        right_parts[:, columns] = right
        jump = stride[:, columns]
        left = right = jnp.zeros_like(jump)
        for s in range(SEGMENTS):
            left = jump * left + left_parts[s : s + 1, columns]
            right = jump * right + right_parts[SEGMENTS - 1 - s : SEGMENTS - s, columns]
        moments[0:1, columns] = left
        moments[1:2, columns] = right


def forward_kernel(
    groups, pitch, early, source, screening, constants, cosines,
    table_high, table_low, partial, next_high, next_low,
    last_spectrum, last_left, last_right, last_moments, coefficients,
    angles, angle_sems, cosines_here, cosines_sem, stage, arrived, high, low, back_high, back_low,
    spectrum, left_parts, right_parts, left_states, right_states,
    landed, send_sems, recv_sems,
):
    _, steps, length = source.shape
    rows = SEGMENTS * steps
    half = length // 2
    blocks = length // LANES
    tiles = half // TILE
    last = tiles - 1
    position = lax.axis_index(GRID_AXES)

    angle_copies = [
        pltpu.make_async_copy(
            constants.at[:, pl.ds(t * TILE, TILE)], angles.at[:, pl.ds(t * TILE, TILE)], angle_sems.at[t]
        )
        for t in range(tiles)
    ]
    cosines_copy = pltpu.make_async_copy(cosines, cosines_here, cosines_sem.at[0])
    copies = [
        pltpu.make_async_copy(
            source.at[:, :, pl.ds(c * LANES, LANES)],
            stage.at[c].reshape(SEGMENTS, pitch, LANES).at[:, pl.ds(0, steps), :],
            arrived.at[c],
        )
        for c in range(blocks)
    ]
    angle_copies[0].start()
    cosines_copy.start()
    for c in range(blocks // 2):
        copies[c].start()
        copies[blocks - 1 - c].start()
    for copy in angle_copies[1:]:
        copy.start()
    barrier = pltpu.get_barrier_semaphore()
    for d in range(1, groups):
        pl.semaphore_signal(barrier, inc=1, device_id=peer((position + d) % groups), device_id_type=MESH)

    coarse_rows = half // STEP

    def make_table(t):
        columns = tile_columns(t)
        fine_sin = angles[2 * coarse_rows : 2 * coarse_rows + STEP, columns]
        fine_cos = angles[2 * coarse_rows + STEP : 2 * coarse_rows + 2 * STEP, columns]
        for a in range(coarse_rows):
            coarse_sin = angles[a : a + 1, columns]
            coarse_cos = angles[coarse_rows + a : coarse_rows + a + 1, columns]
            place = slice(a * STEP, (a + 1) * STEP)
            table_high[place, columns], table_low[place, columns] = split(coarse_sin * fine_cos + coarse_cos * fine_sin)

    def row_of(index, t):
        return coefficients[index, t : t + 1, :]

    angle_copies[0].wait()
    cosines_copy.wait()
    store_coefficients(groups, rows, screening[0], cosines_here[...], coefficients)
    make_table(0)
    signs = parity((2 * SEGMENTS, LANES))
    pairs = blocks // 2
    size = max(pairs // FOLDS, 1)
    for begin in range(0, pairs, size):
        chosen = range(begin, min(begin + size, pairs))
        for c in chosen:
            copies[c].wait()
            copies[blocks - 1 - c].wait()
        if begin + size >= pairs:
            for copy in angle_copies[1:]:
                copy.wait()
            pl.semaphore_wait(barrier, groups - 1)
        for c in chosen:
            columns = pl.ds(c * LANES, LANES)
            for g in range(0, steps, 2):
                place = pl.ds(g * SEGMENTS, 2 * SEGMENTS)
                place_sum = pl.ds(rows + g * SEGMENTS, 2 * SEGMENTS)

                def load(column):
                    pair = [stage[column, pl.ds(g + e, SEGMENTS, stride=pitch), :] for e in range(2)]
                    return jnp.concatenate(pair, axis=0)

                near = load(c)
                far = mirrored(load(blocks - 1 - c))
                high[place, columns], low[place, columns] = split(near - far)
                high[place_sum, columns], low[place_sum, columns] = split((near + far) * signs)
    def lines_of(t):
        return last_spectrum if t == last else spectrum.at[t]

    def sums_of(t):
        return (last_left, last_right) if t == last else (left_parts.at[t], right_parts.at[t])

    def transform(t, h):
        columns = tile_columns(t)
        for k in range(2):
            part = slice(k * rows // 2, (k + 1) * rows // 2)
            place = slice(h * rows + k * rows // 2, h * rows + (k + 1) * rows // 2)
            lines_of(t)[part, tile_columns(h)] = product(
                high[place, :], low[place, :], table_high[:, columns], table_low[:, columns]
            )

    every = (0, 1)
    whole_tile = slice(0, 2 * TILE)

    def sum_lines(t):
        line_sums(lines_of(t), row_of(0, t), row_of(1, t), *sums_of(t), landed.at[t, 0])

    def send(t):
        for d in range(1, groups):
            pltpu.make_async_remote_copy(
                src_ref=landed.at[t, 0],
                dst_ref=landed.at[t, d],
                send_sem=send_sems.at[t],
                recv_sem=recv_sems.at[t],
                device_id=peer((position + d) % groups),
                device_id_type=MESH,
            ).start()

    def all_of(t):
        ref = landed.at[t, pl.ds(1, groups - 1)]
        return pltpu.make_async_remote_copy(
            src_ref=ref,
            dst_ref=ref,
            send_sem=send_sems.at[t],
            recv_sem=recv_sems.at[t],
            device_id=peer((position + 1) % groups),
            device_id_type=MESH,
        )

    for t in range(tiles):
        transform(t, 0)
        if t:
            sum_lines(t - 1)
            send(t - 1)
        transform(t, 1)
        if t < last:
            make_table(t + 1)
    sum_lines(last)
    send(last)

    def multiply(t, high, low, chosen):
        inner = slice(t * TILE, (t + 1) * TILE)
        for n in chosen:
            columns = tile_columns(n)
            for h in every:
                place = slice(h * rows, (h + 1) * rows)
                values = product(high[place, :], low[place, :], table_high[inner, columns], table_low[inner, columns])
                partial[place, columns] = values if t == 0 else partial[place, columns] + values

    def target_of(t):
        return (next_high, next_low) if t == last - 1 else (back_high.at[t], back_low.at[t])

    for t in range(last):
        all_of(t).wait_recv()
        if t:
            multiply(t - 1, *target_of(t - 1), (tiles - 1,))
        boundary_states(
            groups, lambda index: landed[t, index], [row_of(i, t) for i in range(COEFFICIENTS)],
            *sums_of(t), left_states.at[t], right_states.at[t], whole_tile,
        )
        solve_lines(lines_of(t), row_of(0, t), left_states.at[t], right_states.at[t], *target_of(t))
        multiply(t, *target_of(t), range(early if t == last - 1 else tiles - 1))
    all_of(last).wait_recv()
    for d in range(groups):
        last_moments[d] = landed[last, d]
    for t in range(tiles):
        all_of(t).wait_send()


def backward_kernel(
    groups, pitch, early, table_high, table_low, partial, next_high, next_low,
    last_spectrum, last_left, last_right, last_moments, coefficients,
    solved, acc, last_high, last_low, left_states, right_states, stage, stored,
):
    _, steps, length = solved.shape
    rows = SEGMENTS * steps
    half = length // 2
    blocks = length // LANES
    tiles = half // TILE
    last = tiles - 1

    def multiply(t, high, low, base, n):
        columns = tile_columns(n)
        inner = slice(t * TILE, (t + 1) * TILE)
        values = []
        for h in range(2):
            place = slice(h * rows, (h + 1) * rows)
            values.append(
                base[place, columns]
                + product(high[place, :], low[place, :], table_high[inner, columns], table_low[inner, columns])
            )
        return values

    for n in range(early, tiles):
        acc[:rows, tile_columns(n)], acc[rows:, tile_columns(n)] = multiply(last - 1, next_high, next_low, partial, n)
    row_values = [coefficients[i, last:tiles, :] for i in range(COEFFICIENTS)]
    boundary_states(
        groups, lambda index: last_moments[index], row_values,
        last_left, last_right, left_states, right_states, slice(0, 2 * TILE),
    )
    solve_lines(last_spectrum, row_values[0], left_states, right_states, last_high, last_low)
    signs = parity((SEGMENTS, LANES))
    copies = []
    ready = []

    def store(near):
        for index in (near, blocks - 1 - near):
            copy = pltpu.make_async_copy(
                stage.at[index].reshape(SEGMENTS, pitch, LANES).at[:, pl.ds(0, steps), :],
                solved.at[:, :, pl.ds(index * LANES, LANES)],
                stored.at[index],
            )
            copy.start()
            copies.append(copy)

    for n in range(tiles):
        while len(ready) < min(n + AHEAD, tiles):
            m = len(ready)
            ready.append(multiply(last, last_high, last_low, partial if m < early else acc, m))
        odds, evens = ready[n]
        for c in range(TILE // LANES):
            near = n * TILE // LANES + c
            far = blocks - 1 - near
            lanes = slice(c * LANES, (c + 1) * LANES)
            for g in range(steps):
                place = pl.ds(g, SEGMENTS, stride=pitch)
                odd = odds[g * SEGMENTS : (g + 1) * SEGMENTS, lanes]
                even = evens[g * SEGMENTS : (g + 1) * SEGMENTS, lanes] * signs
                stage[near, place, :] = even + odd
                stage[far, place, :] = mirrored(even - odd)
        for c in range(TILE // LANES):
            store(n * TILE // LANES + c)
    for copy in copies:
        copy.wait()


def on_device(source, screening):
    groups = lax.axis_size(GRID_AXES)
    fields, rows, length = source.shape
    half = length // 2
    tiles = half // TILE
    width = 2 * TILE
    steps = rows // SEGMENTS
    pitch = steps + 8 if steps % 16 == 0 else steps
    blocks = length // LANES
    constants = jnp.asarray(constant_rows(length))
    cosines = jnp.asarray(cosine_rows(length))
    vmem = pl.BlockSpec(memory_space=pltpu.VMEM)
    hbm = pl.BlockSpec(memory_space=pl.ANY)
    f32 = lambda *shape: jax.ShapeDtypeStruct(shape, jnp.float32)
    bf16 = lambda *shape: jax.ShapeDtypeStruct(shape, jnp.bfloat16)
    stay = lambda array: pltpu.with_memory_space_constraint(array, pltpu.HBM)
    floats = lambda *shape: pltpu.VMEM(shape, jnp.float32)
    halves = lambda *shape: pltpu.VMEM(shape, jnp.bfloat16)
    staging = [floats(blocks, SEGMENTS * pitch, LANES), pltpu.SemaphoreType.DMA((blocks,))]

    def one_field(grid, constant):
        parts = pl.pallas_call(
            functools.partial(forward_kernel, groups, pitch, tiles // 2),
            out_shape=[
                bf16(half, half), bf16(half, half), f32(2 * rows, half),
                bf16(2 * rows, TILE), bf16(2 * rows, TILE),
                f32(rows, width), f32(SEGMENTS, width), f32(SEGMENTS, width),
                f32(groups, 2, width), f32(COEFFICIENTS, *cosines.shape),
            ],
            in_specs=[hbm, pl.BlockSpec(memory_space=pltpu.SMEM), hbm, hbm],
            out_specs=[vmem] * 10,
            scratch_shapes=[
                floats(*constants.shape), pltpu.SemaphoreType.DMA((tiles,)),
                floats(*cosines.shape), pltpu.SemaphoreType.DMA((1,)),
            ]
            + staging
            + [halves(2 * rows, half)] * 2
            + [halves(tiles - 1, 2 * rows, TILE)] * 2
            + [floats(tiles - 1, rows, width)]
            + [floats(tiles - 1, SEGMENTS, width)] * 4
            + [floats(tiles, groups, 2, width)]
            + [pltpu.SemaphoreType.DMA((tiles,))] * 2,
            compiler_params=pltpu.CompilerParams(
                vmem_limit_bytes=40 * 2**20, collective_id=0, has_side_effects=True
            ),
            name="forward",
        )(stay(grid.reshape(SEGMENTS, steps, length)), constant, stay(constants), stay(cosines))
        solved = pl.pallas_call(
            functools.partial(backward_kernel, groups, pitch, tiles // 2),
            out_shape=f32(SEGMENTS, steps, length),
            in_specs=[vmem] * 10,
            out_specs=hbm,
            scratch_shapes=[floats(2 * rows, half)]
            + [halves(2 * rows, TILE)] * 2
            + [floats(SEGMENTS, width)] * 2
            + staging,
            compiler_params=pltpu.CompilerParams(vmem_limit_bytes=40 * 2**20),
            name="backward",
        )(*parts)
        return solved.reshape(rows, length)

    return jnp.stack([one_field(source[f], screening[f : f + 1]) for f in range(fields)])


def solution(mesh):
    return jax.shard_map(
        on_device,
        mesh=mesh,
        in_specs=(P("af", GRID_AXES, None), P("af")),
        out_specs=P("af", GRID_AXES, None),
        check_vma=False,
    )
```
